32 devices in a mesh: zero: 8 (over z, y), width: 4 (over x, core).
Axes of the slice: x: 2, y: 2, z: 4, core: 2. Of those that a mesh axis runs over, the one named last changes fastest.
Arguments:
- train_query: float32 [7168, 7168], P('zero', 'width'), may hold values from -0.09375 to 0.09375
- slow_query: float32 [7168, 7168], P('zero', 'width'), may hold values from -0.0625 to 0.0625
- train_key: float32 [7168, 1024], P('zero', 'width'), may hold values from -0.09375 to 0.09375
- slow_key: float32 [7168, 1024], P('zero', 'width'), may hold values from -0.0625 to 0.0625
- train_value: float32 [7168, 1024], P('zero', 'width'), may hold values from -0.09375 to 0.09375
- slow_value: float32 [7168, 1024], P('zero', 'width'), may hold values from -0.0625 to 0.0625
- norm_train: float32 [7168], P(('zero', 'width')), may hold values from 0.25 to 1.75
- norm_step: float32 [7168], P(('zero', 'width')), may hold values from -0.3 to 0.3
Outputs:
- ready_query: bfloat16 [7168, 7168], P(None, 'width')
- ready_key: bfloat16 [7168, 1024], P(None, 'width')
- ready_value: bfloat16 [7168, 1024], P(None, 'width')
- scale_query: float32 [7168], P('width')
- scale_key: float32 [1024], P('width')
- scale_value: float32 [1024], P('width')
- serve_norm: bfloat16 [7168], replicated
- latest_query: float32 [7168, 7168], P('zero', 'width')
- latest_key: float32 [7168, 1024], P('zero', 'width')
- latest_value: float32 [7168, 1024], P('zero', 'width')
The draws below stay inside these ranges and needn't reach their ends.
All inputs are finite; a program needn't handle non-finite values.
Results may differ from the reference program's by a relative error of at most 0.0004.
Values may be sent and summed in bfloat16 or wider, within the bound.
A program may use at most 128 MiB of HBM per device.

```python
import jax
import jax.numpy as jnp
from jax import lax

D_MODEL = 7168
Q_DIM = 7168
KV_DIM = 1024


def strengthened(result, key, source, target, blocks, factor):
    def block_of(dim):
        return (jnp.arange(result.shape[dim]) // (result.shape[dim] // blocks)).reshape((-1,) + (1,) * (result.ndim - 1 - dim))

    near = jax.random.permutation(key, blocks)[block_of(target)]
    far = (block_of(target) + blocks // 2) % blocks
    return jnp.where((block_of(source) == near) | (block_of(source) == far), factor * result, result)


def levels(stream_key, extent, shards, smallest, high):
    def one(position, parts):
        heights = jax.random.uniform(jax.random.fold_in(jax.random.fold_in(stream_key, 6), position), (parts,), jnp.float32, smallest / len(shards), high / len(shards))
        return jnp.repeat(jnp.exp(heights), extent[position] // parts).reshape((-1,) + (1,) * (len(extent) - position - 1))

    factor_of = one(*shards[0])
    for cut in shards[1:]:
        factor_of = factor_of * one(*cut)
    return factor_of


def bell_draw(rng, extent, deviation, limit, shards=(), kind=jnp.bfloat16):
    entries = deviation * jax.random.normal(rng, extent, jnp.float32)
    if shards:
        entries = entries * levels(rng, extent, shards, -0.22, 0.18)
    return jnp.clip(entries, -limit, limit).astype(kind)


def noise_with(own_key, dims, deviation, bound, pieces, heavy, dtype=jnp.bfloat16):
    entries = deviation * jax.random.normal(own_key, dims, jnp.float32)
    if pieces:
        entries = entries * levels(own_key, dims, pieces, -0.22, 0.18)
    return jnp.clip(strengthened(entries, jax.random.fold_in(own_key, 3), *heavy), -bound, bound).astype(dtype)


def setup_inputs(seed: int = 0) -> dict:
    seeds = jax.random.split(jax.random.key(seed), 9)
    train_query = noise_with(seeds[0], (D_MODEL, Q_DIM), D_MODEL ** -0.5, 0.09375, ((0, 8), (1, 4)), (0, 1, 8, 2.0), jnp.float32)
    slow_query = bell_draw(seeds[1], (D_MODEL, Q_DIM), D_MODEL ** -0.5, 0.0625, ((0, 8), (1, 4)), jnp.float32)
    train_key = noise_with(seeds[2], (D_MODEL, KV_DIM), D_MODEL ** -0.5, 0.09375, ((0, 8), (1, 4)), (0, 1, 8, 2.0), jnp.float32)
    slow_key = bell_draw(seeds[3], (D_MODEL, KV_DIM), D_MODEL ** -0.5, 0.0625, ((0, 8), (1, 4)), jnp.float32)
    train_value = noise_with(seeds[4], (D_MODEL, KV_DIM), D_MODEL ** -0.5, 0.09375, ((0, 8), (1, 4)), (0, 1, 8, 2.0), jnp.float32)
    slow_value = bell_draw(seeds[5], (D_MODEL, KV_DIM), D_MODEL ** -0.5, 0.0625, ((0, 8), (1, 4)), jnp.float32)
    norm_train = jnp.clip(1.0 + 0.15 * jax.random.normal(seeds[6], (D_MODEL,), jnp.float32), 0.25, 1.75)
    norm_step = jnp.clip(jax.random.uniform(seeds[7], (D_MODEL,), jnp.float32, -0.3, 0.3) * levels(seeds[7], (D_MODEL,), ((0, 32),), -0.4, 0.0), -0.3, 0.3)
    return {"train_query": train_query, "slow_query": slow_query, "train_key": train_key, "slow_key": slow_key, "train_value": train_value, "slow_value": slow_value, "norm_train": norm_train, "norm_step": norm_step}


keep_rate = 0.5

def reference(train_query, slow_query, train_key, slow_key, train_value, slow_value, norm_train, norm_step):
    latest_query = keep_rate * slow_query + (1.0 - keep_rate) * train_query
    latest_key = keep_rate * slow_key + (1.0 - keep_rate) * train_key
    latest_value = keep_rate * slow_value + (1.0 - keep_rate) * train_value
    scale_query = jnp.sqrt(lax.optimization_barrier(jnp.sum(latest_query * latest_query, axis=0)))
    ready_query = (latest_query / scale_query).astype(jnp.bfloat16)
    scale_key = jnp.sqrt(lax.optimization_barrier(jnp.sum(latest_key * latest_key, axis=0)))
    ready_key = (latest_key / scale_key).astype(jnp.bfloat16)
    scale_value = jnp.sqrt(lax.optimization_barrier(jnp.sum(latest_value * latest_value, axis=0)))
    ready_value = (latest_value / scale_value).astype(jnp.bfloat16)
    serve_norm = (norm_train + norm_step).astype(jnp.bfloat16)
    return (ready_query, ready_key, ready_value, scale_query, scale_key, scale_value, serve_norm, latest_query, latest_key, latest_value)
```

```python
import functools

import jax
import jax.numpy as jnp
from jax import lax
from jax.experimental import pallas as pl
from jax.experimental.pallas import tpu as pltpu
from jax.sharding import PartitionSpec as P

keep_rate = 0.5
MESH = pl.DeviceIdType.MESH


def grid_of(count):
    fast = 1
    while (2 * fast) ** 2 <= count and count % (2 * fast) == 0:
        fast *= 2
    return count // fast, fast


def node_at(place, slow, fast):
    if fast == 1:
        return place
    deep = slow - 1
    back = place // (deep * fast)
    column = place // deep
    step = place % deep
    step = step + (column % 2) * (deep - 1 - 2 * step)
    z = (1 - back) * (1 + step)
    y = (1 - back) * column + back * (fast - 1 - (place - deep * fast))
    return z * fast + y


def place_of(node, slow, fast):
    if fast == 1:
        return node
    deep = slow - 1
    z, y = node // fast, node % fast
    out = (z + slow - 1) // slow
    step = z - 1
    step = step + (y % 2) * (deep - 1 - 2 * step)
    return out * (y * deep + step) + (1 - out) * (deep * fast + fast - 1 - y)


def ring_of(count):
    me = lax.axis_index("zero")
    slow, fast = grid_of(count)
    place = place_of(me, slow, fast)

    def node(step):
        return node_at(lax.rem(place + count + step, count), slow, fast)

    return me, node


def gather_kernel(
    count, across, width, half, tile, groups, parts,
    tq, sq, tk, sk, tv, sv, norm_train, norm_step,
    rq, rk, rv, lq, lk, lv, scale_q, scale_k, scale_v, norm_all,
    itq, isq, itk, isk, itv, isv, stats,
    load_sem, stat_send, stat_recv, near_send, near_recv, far_send, far_recv,
    send_sem, recv_sem,
):
    me, node = ring_of(count)
    side = lax.axis_index("width")
    late = lax.rem(side, 2) == 0
    ahead, behind = node(1), node(-1)
    rows = 2 * half
    trains, slows = ((tq, itq), (tk, itk), (tv, itv)), ((sq, isq), (sk, isk), (sv, isv))
    latest, ready, scales = (lq, lk, lv), (rq, rk, rv), (scale_q, scale_k, scale_v)

    def columns(c):
        return pl.ds(c * width, width)

    def early(i, action):
        if groups[i][0] == 2:
            pl.when(jnp.logical_not(late))(action)
        else:
            action()

    barrier = pltpu.get_barrier_semaphore()
    for k in range(1, count):
        pl.semaphore_signal(
            barrier, inc=1, device_id=(lax.rem(me + k, count), side), device_id_type=MESH
        )
    for k in range(1, across):
        pl.semaphore_signal(
            barrier, inc=1, device_id=(me, lax.rem(side + k, across)), device_id_type=MESH
        )

    loads = []
    for i, (which, c) in enumerate(groups):
        pair = []
        for j, arrays in enumerate((trains, slows)):
            far, near = arrays[which]
            pair.append(
                pltpu.make_async_copy(far.at[:, columns(c)], near.at[:, columns(c)], load_sem.at[j, i])
            )
            pair[-1].start()
        loads.append(pair)
    mine = me * across + side
    norm_all[mine] = norm_train[...] + norm_step[...]

    def stat_copy(part, k):
        first, last = parts[part]
        piece = stats.at[me, :, pl.ds(first * width, (last - first) * width)]
        return pltpu.make_async_remote_copy(
            src_ref=piece, dst_ref=piece,
            send_sem=stat_send.at[part, k - 1], recv_sem=stat_recv.at[part, k - 1],
            device_id=(lax.rem(me + k, count), side), device_id_type=MESH,
        )

    def near_copy(k):
        return pltpu.make_async_remote_copy(
            src_ref=norm_all.at[mine], dst_ref=norm_all.at[mine],
            send_sem=near_send.at[k - 1], recv_sem=near_recv.at[k - 1],
            device_id=(me, lax.rem(side + k, across)), device_id_type=MESH,
        )

    def far_copy(k):
        at = pl.ds(me * across, across)
        return pltpu.make_async_remote_copy(
            src_ref=norm_all.at[at], dst_ref=norm_all.at[at],
            send_sem=far_send.at[k - 1], recv_sem=far_recv.at[k - 1],
            device_id=(lax.rem(me + k, count), side), device_id_type=MESH,
        )

    def average(i):
        which, c = groups[i]
        for load in loads[i]:
            load.wait()

        def step(t, total):
            at = pl.ds(pl.multiple_of(t * tile, 16), tile)
            value = (
                keep_rate * slows[which][1][at, columns(c)]
                + (1.0 - keep_rate) * trains[which][1][at, columns(c)]
            )
            latest[which][at, columns(c)] = value
            return total + jnp.sum((value * value).reshape(tile // 8, 8, width), axis=0)

        total = lax.fori_loop(0, rows // tile, step, jnp.zeros((8, width), jnp.float32))
        stats[me, :, columns(i)] = jnp.sum(total, axis=0, keepdims=True)

    def ring_copy(owner, step, i, way):
        which, c = groups[i]
        spot = pl.ds(pl.multiple_of(owner * rows + way * half, 16), half)
        piece = ready[which].at[spot, columns(c)]
        return pltpu.make_async_remote_copy(
            src_ref=piece, dst_ref=piece,
            send_sem=send_sem.at[way, step, i], recv_sem=recv_sem.at[way, step, i],
            device_id=(behind if way else ahead, side), device_id_type=MESH,
        )

    def owner_of(step, way):
        return node(step if way else -step)

    def send_own(i):
        which, c = groups[i]
        scale = scales[which][:, columns(c)]
        for way in range(2):

            def step(t, carry):
                at = pl.multiple_of(way * half + t * tile, 16)
                home = pl.multiple_of(me * rows + at, 16)
                ready[which][pl.ds(home, tile), columns(c)] = (
                    latest[which][pl.ds(at, tile), columns(c)] / scale
                ).astype(jnp.bfloat16)
                return carry

            lax.fori_loop(0, half // tile, step, 0)
            early(i, lambda: ring_copy(me, 0, i, way).start())

    def tell(part):
        for k in range(1, count):
            stat_copy(part, k).start()

    def finish(part):
        first, last = parts[part]
        for k in range(1, count):
            stat_copy(part, k).wait_recv()
        for i in range(first, last):
            which, c = groups[i]
            total = stats[0, :, columns(i)]
            for k in range(1, count):
                total = total + stats[k, :, columns(i)]
            scales[which][:, columns(c)] = jnp.sqrt(total)

    for part, (first, last) in enumerate(parts):
        for i in range(first, last):
            average(i)
        if part == 0:
            pl.semaphore_wait(barrier, count + across - 2)
        tell(part)
        if part == 0:
            for k in range(1, across):
                near_copy(k).start()
        else:
            finish(part - 1)
            for i in range(*parts[part - 1]):
                send_own(i)
    finish(len(parts) - 1)
    for i in range(*parts[-1]):
        send_own(i)
    for k in range(1, across):
        near_copy(k).wait_recv()
    for k in range(1, count):
        far_copy(k).start()

    def forward(step, carry):
        owners = owner_of(step, 0), owner_of(step, 1)
        for i in range(len(groups)):

            def pass_on():
                for way in range(2):
                    ring_copy(owners[way], step - 1, i, way).wait_recv()
                    ring_copy(owners[way], step, i, way).start()

            early(i, pass_on)
        return carry

    lax.fori_loop(1, count - 1, forward, 0)
    for i in range(len(groups)):

        def arrive():
            for way in range(2):
                ring_copy(owner_of(count - 1, way), count - 2, i, way).wait_recv()

        early(i, arrive)

    def drain(step, carry):
        for i in range(len(groups)):

            def leave():
                for way in range(2):
                    ring_copy(owner_of(step, way), step, i, way).wait_send()

            early(i, leave)
        return carry

    lax.fori_loop(0, count - 1, drain, 0)
    for k in range(1, count):
        for part in range(len(parts)):
            stat_copy(part, k).wait_send()
        far_copy(k).wait()
    for k in range(1, across):
        near_copy(k).wait_send()


def gather(arrays, norm_train, norm_step, count, across):
    rows = arrays[0].shape[0]
    wides = [a.shape[1] for a in arrays[::2]]
    half = rows // 2
    width = wides[1]
    tile = 112 if half % 112 == 0 else 16
    groups = [(1, 0)] + [(0, c) for c in range(wides[0] // width)] + [(2, 0)]
    n = len(groups)
    parts = [(0, 2), (2, 5), (5, n)]
    piece = norm_train.shape[0]
    hbm = pl.BlockSpec(memory_space=pl.ANY)
    vmem = pl.BlockSpec(memory_space=pltpu.VMEM)
    dma = pltpu.SemaphoreType.DMA
    return pl.pallas_call(
        functools.partial(gather_kernel, count, across, width, half, tile, groups, parts),
        in_specs=[hbm] * 6 + [vmem] * 2,
        out_specs=[vmem] * 10,
        out_shape=[pltpu.VMEM((count * rows, w), jnp.bfloat16) for w in wides]
        + [pltpu.VMEM((rows, w), jnp.float32) for w in wides]
        + [pltpu.VMEM((1, w), jnp.float32) for w in wides]
        + [pltpu.VMEM((count * across, 1, piece), jnp.float32)],
        scratch_shapes=[pltpu.VMEM(a.shape, jnp.float32) for a in arrays]
        + [
            pltpu.VMEM((count, 1, n * width), jnp.float32),
            dma((2, n)),
            dma((len(parts), count - 1)),
            dma((len(parts), count - 1)),
            dma((across - 1,)),
            dma((across - 1,)),
            dma((count - 1,)),
            dma((count - 1,)),
            dma((2, count - 1, n)),
            dma((2, count - 1, n)),
        ],
        compiler_params=pltpu.CompilerParams(
            collective_id=0, has_side_effects=True,
            vmem_limit_bytes=4 * sum(a.size for a in arrays) + 2**21,
        ),
    )(*arrays, norm_train.reshape(1, piece), norm_step.reshape(1, piece))


def pieces_of(source, target, sem, cuts):
    size = source.shape[0] // cuts
    copies = []
    for c in range(cuts):
        at = pl.ds(c * size, size)
        copies.append(pltpu.make_async_copy(source.at[at], target.at[at], sem.at[c]))
    return copies


def store_kernel(
    count, cuts,
    rk, rv, lq, lk, lv, scale_q, scale_k, scale_v, norm, rq,
    out_rk, out_rv, out_lq, out_lk, out_lv, out_sq, out_sk, out_sv, out_norm,
    sem, own_sem,
):
    late = lax.rem(lax.axis_index("width"), 2) == 0
    copies = []
    pairs = ((lq, out_lq), (rk, out_rk), (lk, out_lk), (lv, out_lv))
    for i, (source, target) in enumerate(pairs):
        copies += pieces_of(source, target, sem.at[i], cuts)
    for copy in copies:
        copy.start()
    size = rv.shape[0] // count
    at = pl.ds(pl.multiple_of(lax.axis_index("zero") * size, 16), size)
    own = pltpu.make_async_copy(rv.at[at], out_rv.at[at], own_sem)
    whole = pieces_of(rv, out_rv, sem.at[len(pairs)], cuts)

    @pl.when(late)
    def _():
        own.start()

    @pl.when(jnp.logical_not(late))
    def _():
        for copy in whole:
            copy.start()

    for source, target in ((scale_q, out_sq), (scale_k, out_sk), (scale_v, out_sv)):
        target[...] = source[0, :]
    out_norm[...] = norm[...].astype(jnp.bfloat16)
    for copy in copies:
        copy.wait()

    @pl.when(late)
    def _():
        own.wait()

    @pl.when(jnp.logical_not(late))
    def _():
        for copy in whole:
            copy.wait()


def store(arrays, count):
    cuts = 8
    hbm = pl.BlockSpec(memory_space=pltpu.HBM)
    vmem = pl.BlockSpec(memory_space=pltpu.VMEM)
    return pl.pallas_call(
        functools.partial(store_kernel, count, cuts),
        in_specs=[vmem] * (len(arrays) - 1) + [hbm],
        out_specs=[hbm] * 5 + [vmem] * 4,
        out_shape=[jax.ShapeDtypeStruct(a.shape, a.dtype) for a in arrays[:5]]
        + [jax.ShapeDtypeStruct((a.shape[1],), a.dtype) for a in arrays[5:8]]
        + [jax.ShapeDtypeStruct(arrays[8].shape, jnp.bfloat16)],
        scratch_shapes=[pltpu.SemaphoreType.DMA((5, cuts)), pltpu.SemaphoreType.DMA],
        compiler_params=pltpu.CompilerParams(vmem_limit_bytes=2 * arrays[-1].size + 2**20),
    )(*arrays)


def store_one_kernel(cuts, source, target, sem):
    copies = pieces_of(source, target, sem, cuts)
    for copy in copies:
        copy.start()
    for copy in copies:
        copy.wait()


def store_one(array):
    cuts = 8
    return pl.pallas_call(
        functools.partial(store_one_kernel, cuts),
        in_specs=[pl.BlockSpec(memory_space=pltpu.VMEM)],
        out_specs=pl.BlockSpec(memory_space=pltpu.HBM),
        out_shape=jax.ShapeDtypeStruct(array.shape, array.dtype),
        scratch_shapes=[pltpu.SemaphoreType.DMA((cuts,))],
        compiler_params=pltpu.CompilerParams(vmem_limit_bytes=2**20),
    )(array)


def late_kernel(count, half, cuts, own, after, rv, load_sem, send_sem, recv_sem):
    me, node = ring_of(count)
    side = lax.axis_index("width")
    ahead, behind = node(1), node(-1)
    size = half // cuts

    def ring_copy(owner, step, i, way):
        spot = pl.ds(pl.multiple_of(owner * 2 * half + way * half + i * size, 16), size)
        piece = rv.at[spot]
        return pltpu.make_async_remote_copy(
            src_ref=piece, dst_ref=piece,
            send_sem=send_sem.at[way, step, i], recv_sem=recv_sem.at[way, step, i],
            device_id=(behind if way else ahead, side), device_id_type=MESH,
        )

    def owner_of(step, way):
        return node(step if way else -step)

    @pl.when(lax.rem(side, 2) == 0)
    def _():
        barrier = pltpu.get_barrier_semaphore()
        for other in (ahead, behind):
            pl.semaphore_signal(barrier, inc=1, device_id=(other, side), device_id_type=MESH)
        at = pl.ds(pl.multiple_of(me * 2 * half, 16), 2 * half)
        load = pltpu.make_async_copy(own.at[at], rv.at[at], load_sem)
        load.start()
        load.wait()
        pl.semaphore_wait(barrier, 2)
        for i in range(cuts):
            for way in range(2):
                ring_copy(me, 0, i, way).start()

        def forward(step, carry):
            for i in range(cuts):
                for way in range(2):
                    ring_copy(owner_of(step, way), step - 1, i, way).wait_recv()
                    ring_copy(owner_of(step, way), step, i, way).start()
            return carry

        lax.fori_loop(1, count - 1, forward, 0)
        for i in range(cuts):
            for way in range(2):
                ring_copy(owner_of(count - 1, way), count - 2, i, way).wait_recv()

        def drain(step, carry):
            for i in range(cuts):
                for way in range(2):
                    ring_copy(owner_of(step, way), step, i, way).wait_send()
            return carry

        lax.fori_loop(0, count - 1, drain, 0)


def gather_late(own, after, count):
    half = own.shape[0] // count // 2
    cuts = 7 if half % 112 == 0 else 1
    hbm = pl.BlockSpec(memory_space=pltpu.HBM)
    dma = pltpu.SemaphoreType.DMA
    return pl.pallas_call(
        functools.partial(late_kernel, count, half, cuts),
        in_specs=[hbm, hbm],
        out_specs=pl.BlockSpec(memory_space=pltpu.VMEM),
        out_shape=pltpu.VMEM(own.shape, own.dtype),
        scratch_shapes=[dma, dma((2, count - 1, cuts)), dma((2, count - 1, cuts))],
        compiler_params=pltpu.CompilerParams(
            collective_id=1, has_side_effects=True, vmem_limit_bytes=60 * 2**20
        ),
    )(own, after)


def store_late_kernel(cuts, rv, start, out, sem):
    @pl.when(lax.rem(lax.axis_index("width"), 2) == 0)
    def _():
        copies = pieces_of(rv, out, sem, cuts)
        for copy in copies:
            copy.start()
        for copy in copies:
            copy.wait()


def store_late(rv, start):
    cuts = 8
    hbm = pl.BlockSpec(memory_space=pltpu.HBM)
    return pl.pallas_call(
        functools.partial(store_late_kernel, cuts),
        in_specs=[pl.BlockSpec(memory_space=pltpu.VMEM), hbm],
        out_specs=hbm,
        out_shape=jax.ShapeDtypeStruct(start.shape, start.dtype),
        scratch_shapes=[pltpu.SemaphoreType.DMA((cuts,))],
        input_output_aliases={1: 0},
        compiler_params=pltpu.CompilerParams(vmem_limit_bytes=2**20),
    )(rv, start)


def solution(mesh):
    count, across = mesh.shape["zero"], mesh.shape["width"]

    def body(
        train_query, slow_query, train_key, slow_key, train_value, slow_value, norm_train, norm_step
    ):
        arrays = gather(
            (train_query, slow_query, train_key, slow_key, train_value, slow_value),
            norm_train, norm_step, count, across,
        )
        rq = store_one(arrays[0])
        rk, rv, lq, lk, lv, *scales, norm = store((*arrays[1:], rq), count)
        serve_norm = norm.reshape(-1)
        rv = store_late(gather_late(rv, serve_norm, count), rv)
        return (rq, rk, rv, *scales, serve_norm, lq, lk, lv)

    in_specs = (P("zero", "width"),) * 6 + (P(("zero", "width")),) * 2
    out_specs = (
        (P(None, "width"),) * 3 + (P("width"),) * 3 + (P(),) + (P("zero", "width"),) * 3
    )
    return jax.shard_map(body, mesh=mesh, in_specs=in_specs, out_specs=out_specs, check_vma=False)
```

```python
import functools

import jax
import jax.numpy as jnp
from jax import lax
from jax.experimental import pallas as pl
from jax.experimental.pallas import tpu as pltpu
from jax.sharding import PartitionSpec as P

keep_rate = 0.5
MESH = pl.DeviceIdType.MESH


def grid_of(count):
    fast = 1
    while (2 * fast) ** 2 <= count and count % (2 * fast) == 0:
        fast *= 2
    return count // fast, fast


def node_at(place, slow, fast):
    if fast == 1:
        return place
    deep = slow - 1
    back = place // (deep * fast)
    column = place // deep
    step = place % deep
    step = step + (column % 2) * (deep - 1 - 2 * step)
    z = (1 - back) * (1 + step)
    y = (1 - back) * column + back * (fast - 1 - (place - deep * fast))
    return z * fast + y


def place_of(node, slow, fast):
    if fast == 1:
        return node
    deep = slow - 1
    z, y = node // fast, node % fast
    out = (z + slow - 1) // slow
    step = z - 1
    step = step + (y % 2) * (deep - 1 - 2 * step)
    return out * (y * deep + step) + (1 - out) * (deep * fast + fast - 1 - y)


def ring_of(count):
    me = lax.axis_index("zero")
    slow, fast = grid_of(count)
    place = place_of(me, slow, fast)

    def node(step):
        return node_at(lax.rem(place + count + step, count), slow, fast)

    return me, node


def gather_kernel(
    count, across, width, half, tile, groups, parts, pieces,
    tq, sq, tk, sk, tv, sv, norm_train, norm_step,
    rq, rk, rv, lq, lk, lv, scale_q, scale_k, scale_v, norm_all,
    itq, isq, itk, isk, itv, isv, stats,
    load_sem, stat_send, stat_recv, near_send, near_recv, far_send, far_recv,
    send_sem, recv_sem,
):
    me, node = ring_of(count)
    side = lax.axis_index("width")
    late = lax.rem(side, 2) == 0
    ahead, behind = node(1), node(-1)
    rows = 2 * half
    trains, slows = ((tq, itq), (tk, itk), (tv, itv)), ((sq, isq), (sk, isk), (sv, isv))
    latest, ready, scales = (lq, lk, lv), (rq, rk, rv), (scale_q, scale_k, scale_v)

    def columns(c):
        return pl.ds(c * width, width)

    def allowed(p, action):
        if pieces[p][3]:
            pl.when(jnp.logical_not(late))(action)
        else:
            action()

    barrier = pltpu.get_barrier_semaphore()
    for k in range(1, count):
        pl.semaphore_signal(
            barrier, inc=1, device_id=(lax.rem(me + k, count), side), device_id_type=MESH
        )
    for k in range(1, across):
        pl.semaphore_signal(
            barrier, inc=1, device_id=(me, lax.rem(side + k, across)), device_id_type=MESH
        )

    loads = []
    for i, (which, c) in enumerate(groups):
        pair = []
        for j, arrays in enumerate((trains, slows)):
            far, near = arrays[which]
            pair.append(
                pltpu.make_async_copy(far.at[:, columns(c)], near.at[:, columns(c)], load_sem.at[j, i])
            )
            pair[-1].start()
        loads.append(pair)
    mine = me * across + side
    norm_all[mine] = norm_train[...] + norm_step[...]

    def stat_copy(part, k):
        first, last = parts[part]
        piece = stats.at[me, :, pl.ds(first * width, (last - first) * width)]
        return pltpu.make_async_remote_copy(
            src_ref=piece, dst_ref=piece,
            send_sem=stat_send.at[part, k - 1], recv_sem=stat_recv.at[part, k - 1],
            device_id=(lax.rem(me + k, count), side), device_id_type=MESH,
        )

    def near_copy(k):
        return pltpu.make_async_remote_copy(
            src_ref=norm_all.at[mine], dst_ref=norm_all.at[mine],
            send_sem=near_send.at[k - 1], recv_sem=near_recv.at[k - 1],
            device_id=(me, lax.rem(side + k, across)), device_id_type=MESH,
        )

    def far_copy(k):
        at = pl.ds(me * across, across)
        return pltpu.make_async_remote_copy(
            src_ref=norm_all.at[at], dst_ref=norm_all.at[at],
            send_sem=far_send.at[k - 1], recv_sem=far_recv.at[k - 1],
            device_id=(lax.rem(me + k, count), side), device_id_type=MESH,
        )

    def average(i):
        which, c = groups[i]
        for load in loads[i]:
            load.wait()

        def step(t, total):
            at = pl.ds(pl.multiple_of(t * tile, 16), tile)
            value = (
                keep_rate * slows[which][1][at, columns(c)]
                + (1.0 - keep_rate) * trains[which][1][at, columns(c)]
            )
            latest[which][at, columns(c)] = value
            return total + jnp.sum((value * value).reshape(tile // 8, 8, width), axis=0)

        total = lax.fori_loop(0, rows // tile, step, jnp.zeros((8, width), jnp.float32))
        stats[me, :, columns(i)] = jnp.sum(total, axis=0, keepdims=True)

    def ring_copy(owner, step, p, way):
        i, first, size, _ = pieces[p]
        which, c = groups[i]
        spot = pl.ds(pl.multiple_of(owner * rows + way * half + first, 16), size)
        piece = ready[which].at[spot, columns(c)]
        return pltpu.make_async_remote_copy(
            src_ref=piece, dst_ref=piece,
            send_sem=send_sem.at[way, lax.rem(step, 2), p], recv_sem=recv_sem.at[way, step, p],
            device_id=(behind if way else ahead, side), device_id_type=MESH,
        )

    def owner_of(step, way):
        return node(step if way else -step)

    def send_own(i):
        which, c = groups[i]
        scale = scales[which][:, columns(c)]
        for way in range(2):

            def step(t, carry):
                at = pl.multiple_of(way * half + t * tile, 16)
                home = pl.multiple_of(me * rows + at, 16)
                ready[which][pl.ds(home, tile), columns(c)] = (
                    latest[which][pl.ds(at, tile), columns(c)] / scale
                ).astype(jnp.bfloat16)
                return carry

            lax.fori_loop(0, half // tile, step, 0)
            for p in range(len(pieces)):
                if pieces[p][0] == i:
                    allowed(p, lambda: ring_copy(me, 0, p, way).start())

    def tell(part):
        for k in range(1, count):
            stat_copy(part, k).start()

    def finish(part):
        first, last = parts[part]
        for k in range(1, count):
            stat_copy(part, k).wait_recv()
        for i in range(first, last):
            which, c = groups[i]
            total = stats[0, :, columns(i)]
            for k in range(1, count):
                total = total + stats[k, :, columns(i)]
            scales[which][:, columns(c)] = jnp.sqrt(total)

    for part, (first, last) in enumerate(parts):
        for i in range(first, last):
            average(i)
        if part == 0:
            pl.semaphore_wait(barrier, count + across - 2)
        tell(part)
        if part == 0:
            for k in range(1, across):
                near_copy(k).start()
        else:
            finish(part - 1)
            for i in range(*parts[part - 1]):
                send_own(i)
    finish(len(parts) - 1)
    for i in range(*parts[-1]):
        send_own(i)
    for k in range(1, across):
        near_copy(k).wait_recv()
    for k in range(1, count):
        far_copy(k).start()

    def leave(step):
        for p in range(len(pieces)):

            def left():
                for way in range(2):
                    ring_copy(owner_of(step, way), step, p, way).wait_send()

            allowed(p, left)

    def forward(step, carry):
        owners = owner_of(step, 0), owner_of(step, 1)
        for p in range(len(pieces)):

            def pass_on():
                for way in range(2):
                    ring_copy(owners[way], step - 1, p, way).wait_recv()
                    ring_copy(owners[way], step, p, way).start()

            allowed(p, pass_on)
        leave(step - 1)
        return carry

    lax.fori_loop(1, count - 1, forward, 0)
    for k in range(1, count):
        for part in range(len(parts)):
            stat_copy(part, k).wait_send()
        far_copy(k).wait()
    for k in range(1, across):
        near_copy(k).wait_send()
    for p in range(len(pieces)):

        def arrive():
            for way in range(2):
                ring_copy(owner_of(count - 1, way), count - 2, p, way).wait_recv()

        allowed(p, arrive)
    leave(count - 2)


def cut_of(half):
    return half // 32 * 16


def gather(arrays, norm_train, norm_step, count, across):
    rows = arrays[0].shape[0]
    wides = [a.shape[1] for a in arrays[::2]]
    half = rows // 2
    width = wides[1]
    tile = 112 if half % 112 == 0 else 16
    groups = [(1, 0)] + [(0, c) for c in range(wides[0] // width)] + [(2, 0)]
    n = len(groups)
    cut = cut_of(half)
    pieces = [(i, 0, half, False) for i in range(1, n - 1)]
    pieces = [(0, 0, cut, False), (0, cut, half - cut, True)] + pieces + [(n - 1, 0, half, True)]
    parts = [(0, 2), (2, 5), (5, n)]
    piece = norm_train.shape[0]
    hbm = pl.BlockSpec(memory_space=pl.ANY)
    vmem = pl.BlockSpec(memory_space=pltpu.VMEM)
    dma = pltpu.SemaphoreType.DMA
    return pl.pallas_call(
        functools.partial(gather_kernel, count, across, width, half, tile, groups, parts, pieces),
        in_specs=[hbm] * 6 + [vmem] * 2,
        out_specs=[vmem] * 10,
        out_shape=[pltpu.VMEM((count * rows, w), jnp.bfloat16) for w in wides]
        + [pltpu.VMEM((rows, w), jnp.float32) for w in wides]
        + [pltpu.VMEM((1, w), jnp.float32) for w in wides]
        + [pltpu.VMEM((count * across, 1, piece), jnp.float32)],
        scratch_shapes=[pltpu.VMEM(a.shape, jnp.float32) for a in arrays]
        + [
            pltpu.VMEM((count, 1, n * width), jnp.float32),
            dma((2, n)),
            dma((len(parts), count - 1)),
            dma((len(parts), count - 1)),
            dma((across - 1,)),
            dma((across - 1,)),
            dma((count - 1,)),
            dma((count - 1,)),
            dma((2, 2, len(pieces))),
            dma((2, count - 1, len(pieces))),
        ],
        compiler_params=pltpu.CompilerParams(
            collective_id=0, has_side_effects=True,
            vmem_limit_bytes=4 * sum(a.size for a in arrays) + 2**21,
        ),
    )(*arrays, norm_train.reshape(1, piece), norm_step.reshape(1, piece))


def pieces_of(source, target, sem, cuts):
    size = source.shape[0] // cuts
    copies = []
    for c in range(cuts):
        at = pl.ds(c * size, size)
        copies.append(pltpu.make_async_copy(source.at[at], target.at[at], sem.at[c]))
    return copies


def key_pieces(count, rows, late, small):
    half = rows // 2
    cut = cut_of(half)
    size = half - cut if late else cut
    pieces = []
    for owner in range(count):
        for way in range(2):
            spot = pl.ds(owner * rows + way * half + (cut if late else 0), size)
            pieces.append((pl.ds((owner * 2 + way) * size, size) if small else spot, spot))
    return pieces


def store_kernel(
    count, cuts,
    rk, rv, lq, lk, lv, scale_q, scale_k, scale_v, norm, rq,
    out_rk, out_rv, out_lq, out_lk, out_lv, out_sq, out_sk, out_sv, out_norm,
    sem, key_sem, own_sem,
):
    late = lax.rem(lax.axis_index("width"), 2) == 0
    rows = rv.shape[0] // count
    base = lax.axis_index("zero") * rows
    half = rows // 2
    cut = cut_of(half)
    both, last, first = [], [], []
    for i, (source, target) in enumerate(((lq, out_lq), (lk, out_lk), (lv, out_lv))):
        both += pieces_of(source, target, sem.at[i], cuts)
    first += pieces_of(rk, out_rk, sem.at[3], cuts) + pieces_of(rv, out_rv, sem.at[4], cuts)
    for i, (_, at) in enumerate(key_pieces(count, rows, False, False)):
        last.append(pltpu.make_async_copy(rk.at[at], out_rk.at[at], key_sem.at[i]))
    at = pl.ds(pl.multiple_of(base, 16), rows)
    last.append(pltpu.make_async_copy(rv.at[at], out_rv.at[at], own_sem.at[0]))
    for way in range(2):
        at = pl.ds(pl.multiple_of(base + way * half + cut, 16), half - cut)
        last.append(pltpu.make_async_copy(rk.at[at], out_rk.at[at], own_sem.at[1 + way]))

    for copy in both:
        copy.start()

    @pl.when(late)
    def _():
        for copy in last:
            copy.start()

    @pl.when(jnp.logical_not(late))
    def _():
        for copy in first:
            copy.start()

    for source, target in ((scale_q, out_sq), (scale_k, out_sk), (scale_v, out_sv)):
        target[...] = source[0, :]
    out_norm[...] = norm[...].astype(jnp.bfloat16)
    for copy in both:
        copy.wait()

    @pl.when(late)
    def _():
        for copy in last:
            copy.wait()

    @pl.when(jnp.logical_not(late))
    def _():
        for copy in first:
            copy.wait()


def store(arrays, count):
    cuts = 8
    dma = pltpu.SemaphoreType.DMA
    hbm = pl.BlockSpec(memory_space=pltpu.HBM)
    vmem = pl.BlockSpec(memory_space=pltpu.VMEM)
    return pl.pallas_call(
        functools.partial(store_kernel, count, cuts),
        in_specs=[vmem] * (len(arrays) - 1) + [hbm],
        out_specs=[hbm] * 5 + [vmem] * 4,
        out_shape=[jax.ShapeDtypeStruct(a.shape, a.dtype) for a in arrays[:5]]
        + [jax.ShapeDtypeStruct((a.shape[1],), a.dtype) for a in arrays[5:8]]
        + [jax.ShapeDtypeStruct(arrays[8].shape, jnp.bfloat16)],
        scratch_shapes=[dma((5, cuts)), dma((2 * count,)), dma((3,))],
        compiler_params=pltpu.CompilerParams(vmem_limit_bytes=2 * arrays[-1].size + 2**20),
    )(*arrays)


def store_one_kernel(cuts, source, target, sem):
    copies = pieces_of(source, target, sem, cuts)
    for copy in copies:
        copy.start()
    for copy in copies:
        copy.wait()


def store_one(array):
    cuts = 8
    return pl.pallas_call(
        functools.partial(store_one_kernel, cuts),
        in_specs=[pl.BlockSpec(memory_space=pltpu.VMEM)],
        out_specs=pl.BlockSpec(memory_space=pltpu.HBM),
        out_shape=jax.ShapeDtypeStruct(array.shape, array.dtype),
        scratch_shapes=[pltpu.SemaphoreType.DMA((cuts,))],
        compiler_params=pltpu.CompilerParams(vmem_limit_bytes=2**20),
    )(array)


def late_kernel(count, half, tile, own_k, own_v, after, rk, rv, load_sem, send_sem, recv_sem):
    me, node = ring_of(count)
    side = lax.axis_index("width")
    ahead, behind = node(1), node(-1)
    cut = cut_of(half)
    rest = half - cut
    pieces = [(rk, rest, t * tile) for t in range(rest // tile)]
    pieces += [(rv, half, t * tile) for t in range(half // tile)]

    def ring_copy(owner, step, p, way):
        ref, size, first = pieces[p]
        piece = ref.at[pl.ds(pl.multiple_of((owner * 2 + way) * size + first, 16), tile)]
        return pltpu.make_async_remote_copy(
            src_ref=piece, dst_ref=piece,
            send_sem=send_sem.at[way, lax.rem(step, 2), p], recv_sem=recv_sem.at[way, step, p],
            device_id=(behind if way else ahead, side), device_id_type=MESH,
        )

    def owner_of(step, way):
        return node(step if way else -step)

    def leave(step):
        for p in range(len(pieces)):
            for way in range(2):
                ring_copy(owner_of(step, way), step, p, way).wait_send()

    @pl.when(lax.rem(side, 2) == 0)
    def _():
        barrier = pltpu.get_barrier_semaphore()
        for other in (ahead, behind):
            pl.semaphore_signal(barrier, inc=1, device_id=(other, side), device_id_type=MESH)
        loads = []
        for way in range(2):
            there = pl.ds(pl.multiple_of((me * 2 + way) * half + cut, 16), rest)
            here = pl.ds(pl.multiple_of((me * 2 + way) * rest, 16), rest)
            loads.append(pltpu.make_async_copy(own_k.at[there], rk.at[here], load_sem.at[0, way]))
            at = pl.ds(pl.multiple_of((me * 2 + way) * half, 16), half)
            loads.append(pltpu.make_async_copy(own_v.at[at], rv.at[at], load_sem.at[1, way]))
        for load in loads:
            load.start()
        for load in loads:
            load.wait()
        pl.semaphore_wait(barrier, 2)
        for p in range(len(pieces)):
            for way in range(2):
                ring_copy(me, 0, p, way).start()

        def forward(step, carry):
            for p in range(len(pieces)):
                for way in range(2):
                    ring_copy(owner_of(step, way), step - 1, p, way).wait_recv()
                    ring_copy(owner_of(step, way), step, p, way).start()
            leave(step - 1)
            return carry

        lax.fori_loop(1, count - 1, forward, 0)
        for p in range(len(pieces)):
            for way in range(2):
                ring_copy(owner_of(count - 1, way), count - 2, p, way).wait_recv()
        leave(count - 2)


def gather_late(own_k, own_v, after, count):
    half = own_k.shape[0] // count // 2
    rest = half - cut_of(half)
    tile = 112 if rest % 112 == 0 and half % 112 == 0 else 16
    n = (rest + half) // tile
    hbm = pl.BlockSpec(memory_space=pltpu.HBM)
    vmem = pl.BlockSpec(memory_space=pltpu.VMEM)
    dma = pltpu.SemaphoreType.DMA
    return pl.pallas_call(
        functools.partial(late_kernel, count, half, tile),
        in_specs=[hbm] * 3,
        out_specs=[vmem] * 2,
        out_shape=[
            pltpu.VMEM((2 * count * rest, own_k.shape[1]), own_k.dtype),
            pltpu.VMEM(own_v.shape, own_v.dtype),
        ],
        scratch_shapes=[dma((2, 2)), dma((2, 2, n)), dma((2, count - 1, n))],
        compiler_params=pltpu.CompilerParams(
            collective_id=1, has_side_effects=True, vmem_limit_bytes=56 * 2**20
        ),
    )(own_k, own_v, after)


def store_late_kernel(count, cuts, rk, rv, start_k, start_v, out_k, out_v, sem, key_sem):
    @pl.when(lax.rem(lax.axis_index("width"), 2) == 0)
    def _():
        copies = pieces_of(rv, out_v, sem, cuts)
        for i, (here, there) in enumerate(key_pieces(count, rv.shape[0] // count, True, True)):
            copies.append(pltpu.make_async_copy(rk.at[here], out_k.at[there], key_sem.at[i]))
        for copy in copies:
            copy.start()
        for copy in copies:
            copy.wait()


def store_late(rk, rv, start_k, start_v, count):
    cuts = 8
    hbm = pl.BlockSpec(memory_space=pltpu.HBM)
    vmem = pl.BlockSpec(memory_space=pltpu.VMEM)
    dma = pltpu.SemaphoreType.DMA
    return pl.pallas_call(
        functools.partial(store_late_kernel, count, cuts),
        in_specs=[vmem] * 2 + [hbm] * 2,
        out_specs=[hbm] * 2,
        out_shape=[jax.ShapeDtypeStruct(a.shape, a.dtype) for a in (start_k, start_v)],
        scratch_shapes=[dma((cuts,)), dma((2 * count,))],
        input_output_aliases={2: 0, 3: 1},
        compiler_params=pltpu.CompilerParams(vmem_limit_bytes=40 * 2**20),
    )(rk, rv, start_k, start_v)


def solution(mesh):
    count, across = mesh.shape["zero"], mesh.shape["width"]

    def body(
        train_query, slow_query, train_key, slow_key, train_value, slow_value, norm_train, norm_step
    ):
        arrays = gather(
            (train_query, slow_query, train_key, slow_key, train_value, slow_value),
            norm_train, norm_step, count, across,
        )
        rq = store_one(arrays[0])
        rk, rv, lq, lk, lv, *scales, norm = store((*arrays[1:], rq), count)
        serve_norm = norm.reshape(-1)
        rk, rv = store_late(*gather_late(rk, rv, serve_norm, count), rk, rv, count)
        return (rq, rk, rv, *scales, serve_norm, lq, lk, lv)

    in_specs = (P("zero", "width"),) * 6 + (P(("zero", "width")),) * 2
    out_specs = (
        (P(None, "width"),) * 3 + (P("width"),) * 3 + (P(),) + (P("zero", "width"),) * 3
    )
    return jax.shard_map(body, mesh=mesh, in_specs=in_specs, out_specs=out_specs, check_vma=False)
```

```python
import functools

import jax
import jax.numpy as jnp
from jax import lax
from jax.experimental import pallas as pl
from jax.experimental.pallas import tpu as pltpu
from jax.sharding import PartitionSpec as P

keep_rate = 0.5
MESH = pl.DeviceIdType.MESH


def grid_of(count):
    fast = 1
    while (2 * fast) ** 2 <= count and count % (2 * fast) == 0:
        fast *= 2
    return count // fast, fast


def node_at(place, slow, fast):
    if fast == 1:
        return place
    deep = slow - 1
    back = place // (deep * fast)
    column = place // deep
    step = place % deep
    step = step + (column % 2) * (deep - 1 - 2 * step)
    z = (1 - back) * (1 + step)
    y = (1 - back) * column + back * (fast - 1 - (place - deep * fast))
    return z * fast + y


def place_of(node, slow, fast):
    if fast == 1:
        return node
    deep = slow - 1
    z, y = node // fast, node % fast
    out = (z + slow - 1) // slow
    step = z - 1
    step = step + (y % 2) * (deep - 1 - 2 * step)
    return out * (y * deep + step) + (1 - out) * (deep * fast + fast - 1 - y)


def ring_of(count):
    me = lax.axis_index("zero")
    slow, fast = grid_of(count)
    place = place_of(me, slow, fast)

    def node(step):
        return node_at(lax.rem(place + count + step, count), slow, fast)

    return me, node


def gather_kernel(
    count, across, width, half, tile, raw_rows, parts, batches, pieces,
    tq, sq, tk, sk, tv, sv, norm_train, norm_step,
    rq, rk, rv, lq, lk, lv, scale_q, scale_k, scale_v, norm_all,
    itq, isq, itk, isk, itv, isv, in_train, in_step, stats, raw,
    load_sem, norm_sem, stat_send, stat_recv, near_sem, far_sem, raw_send, raw_recv,
    send_sem, recv_sem,
):
    me, node = ring_of(count)
    side = lax.axis_index("width")
    late = lax.rem(side, 2) == 1
    ahead, behind = node(1), node(-1)
    rows = 2 * half
    trains, slows = ((tq, itq), (tk, itk), (tv, itv)), ((sq, isq), (sk, isk), (sv, isv))
    latest, ready, scales = (lq, lk, lv), (rq, rk, rv), (scale_q, scale_k, scale_v)
    groups = [group for part in parts for group in part]

    def columns(c, n=1):
        return pl.ds(c * width, n * width)

    def allowed(p, action):
        if pieces[p][5]:
            pl.when(jnp.logical_not(late))(action)
        else:
            action()

    barrier = pltpu.get_barrier_semaphore()
    for k in range(1, count):
        pl.semaphore_signal(
            barrier, inc=1, device_id=(lax.rem(me + k, count), side), device_id_type=MESH
        )
    for k in range(1, across):
        pl.semaphore_signal(
            barrier, inc=1, device_id=(me, lax.rem(side + k, across)), device_id_type=MESH
        )

    loads = []
    for i, (_, which, c, n) in enumerate(batches):
        for j, arrays in enumerate((trains, slows)):
            far, near = arrays[which]
            loads.append(
                pltpu.make_async_copy(
                    far.at[:, columns(c, n)], near.at[:, columns(c, n)], load_sem.at[i, j]
                )
            )
            loads[-1].start()
    norms = [
        pltpu.make_async_copy(far, near, norm_sem.at[j])
        for j, (far, near) in enumerate(((norm_train, in_train), (norm_step, in_step)))
    ]
    for load in norms:
        load.start()
    mine = me * across + side

    def part_columns(part):
        first = groups.index(parts[part][0])
        return columns(first, len(parts[part]))

    def stat_copy(part, k):
        piece = stats.at[me, :, part_columns(part)]
        return pltpu.make_async_remote_copy(
            src_ref=piece, dst_ref=piece, send_sem=stat_send.at[0], recv_sem=stat_recv.at[part],
            device_id=(lax.rem(me + k, count), side), device_id_type=MESH,
        )

    def all_stats(part=None):
        piece = stats.at[pl.ds(0, count - 1)]
        if part is not None:
            piece = stats.at[pl.ds(0, count - 1), :, part_columns(part)]
        return pltpu.make_async_remote_copy(
            src_ref=piece, dst_ref=piece, send_sem=stat_send.at[0],
            recv_sem=stat_recv.at[part or 0], device_id=(ahead, side), device_id_type=MESH,
        )

    def near_copy(at, k=1):
        return pltpu.make_async_remote_copy(
            src_ref=norm_all.at[at], dst_ref=norm_all.at[at],
            send_sem=near_sem.at[0], recv_sem=near_sem.at[1],
            device_id=(me, lax.rem(side + k, across)), device_id_type=MESH,
        )

    def far_copy(at, k=1):
        return pltpu.make_async_remote_copy(
            src_ref=norm_all.at[at], dst_ref=norm_all.at[at],
            send_sem=far_sem.at[0], recv_sem=far_sem.at[1],
            device_id=(lax.rem(me + k, count), side), device_id_type=MESH,
        )

    all_near = near_copy(pl.ds(0, across - 1))
    all_far = far_copy(pl.ds(0, (count - 1) * across))

    def average(i):
        which, c = groups[i]

        def step(t, total):
            at = pl.ds(pl.multiple_of(t * tile, 16), tile)
            value = (
                keep_rate * slows[which][1][at, columns(c)]
                + (1.0 - keep_rate) * trains[which][1][at, columns(c)]
            )
            latest[which][at, columns(c)] = value
            return total + jnp.sum((value * value).reshape(tile // 8, 8, width), axis=0)

        total = lax.fori_loop(0, rows // tile, step, jnp.zeros((8, width), jnp.float32))
        stats[me, :, columns(i)] = jnp.sum(total, axis=0, keepdims=True)

    def averages(part):
        for i, batch in enumerate(batches):
            if batch[0] == part:
                loads[2 * i].wait()
                loads[2 * i + 1].wait()
        for group in parts[part]:
            average(groups.index(group))

    def ring_copy(owner, step, p, way):
        which, c, n, first, size, _ = pieces[p]
        spot = pl.ds(pl.multiple_of(owner * rows + way * half + first, 16), size)
        piece = ready[which].at[spot, columns(c, n)]
        return pltpu.make_async_remote_copy(
            src_ref=piece, dst_ref=piece,
            send_sem=send_sem.at[way, lax.rem(step, 2), p],
            recv_sem=recv_sem.at[way, lax.rem(step, 3), p],
            device_id=(behind if way else ahead, side), device_id_type=MESH,
        )

    def raw_copy(way):
        return pltpu.make_async_remote_copy(
            src_ref=lk.at[pl.ds(way * half, raw_rows)], dst_ref=raw.at[way],
            send_sem=raw_send.at[way], recv_sem=raw_recv.at[way],
            device_id=(behind if way else ahead, side), device_id_type=MESH,
        )

    def owner_of(step, way):
        return node(step if way else -step)

    def send_own(part):
        for p, (which, c, n, first, size, _) in enumerate(pieces):
            if (which, c) not in parts[part]:
                continue
            for way in range(2):
                for each in range(c, c + n):
                    scale = scales[which][:, columns(each)]
                    short = tile if size % tile == 0 else 16

                    def step(t, carry):
                        at = pl.multiple_of(way * half + first + t * short, 16)
                        home = pl.multiple_of(me * rows + at, 16)
                        ready[which][pl.ds(home, short), columns(each)] = (
                            latest[which][pl.ds(at, short), columns(each)] / scale
                        ).astype(jnp.bfloat16)
                        return carry

                    lax.fori_loop(0, size // short, step, 0)
                if p:
                    allowed(p, lambda: ring_copy(me, 0, p, way).start())

    def tell(part):
        for k in range(1, count):
            stat_copy(part, k).start()

    def finish(part):
        all_stats(part).wait_recv()
        for group in parts[part]:
            i = groups.index(group)
            which, c = group
            total = stats[0, :, columns(i)]
            for k in range(1, count):
                total = total + stats[k, :, columns(i)]
            scales[which][:, columns(c)] = jnp.sqrt(total)

    for part in range(len(parts)):
        averages(part)
        if part == 0:
            pl.semaphore_wait(barrier, count + across - 2)
        tell(part)
        if part == 0:
            for way in range(2):
                raw_copy(way).start()
            for load in norms:
                load.wait()
            norm_all[mine] = in_train[...] + in_step[...]
            for k in range(1, across):
                near_copy(mine, k).start()
        else:
            finish(part - 1)
            send_own(part - 1)
    finish(len(parts) - 1)
    send_own(len(parts) - 1)
    all_near.wait_recv()
    for k in range(1, count):
        far_copy(pl.ds(me * across, across), k).start()

    def leave(step):
        for p in range(len(pieces)):

            def left():
                for way in range(2):
                    ring_copy(owner_of(step, way), step, p, way).wait_send()

            if p:
                allowed(p, left)
            else:
                pl.when(step > 0)(left)

    def pass_raw():
        short = tile if raw_rows % tile == 0 else 16
        for way in range(2):
            raw_copy(way).wait_recv()
            home = owner_of(1, way) * rows + way * half

            def step(t, carry):
                at = pl.ds(pl.multiple_of(t * short, 16), short)
                rk[pl.ds(pl.multiple_of(home + t * short, 16), short), :] = (
                    raw[way, at, :] / scale_k[...]
                ).astype(jnp.bfloat16)
                return carry

            lax.fori_loop(0, raw_rows // short, step, 0)
            ring_copy(owner_of(1, way), 1, 0, way).start()

    def forward(step, carry):
        owners = owner_of(step, 0), owner_of(step, 1)
        for p in range(len(pieces)):

            def pass_on():
                for way in range(2):
                    ring_copy(owners[way], step - 1, p, way).wait_recv()
                    ring_copy(owners[way], step, p, way).start()

            if p:
                allowed(p, pass_on)
            else:
                pl.when(step > 1)(pass_on)
        leave(step - 1)
        return carry

    pass_raw()
    lax.fori_loop(1, count - 1, forward, 0)
    for way in range(2):
        raw_copy(way).wait_send()
    all_stats().wait_send()
    all_near.wait_send()
    all_far.wait_send()
    all_far.wait_recv()
    for p in range(len(pieces)):

        def arrive():
            for way in range(2):
                ring_copy(owner_of(count - 1, way), count - 2, p, way).wait_recv()

        allowed(p, arrive)
    leave(count - 2)


def cut_of(half):
    return half // 32 * 16


def gather(arrays, norm_train, norm_step, count, across):
    rows = arrays[0].shape[0]
    wides = [a.shape[1] for a in arrays[::2]]
    half = rows // 2
    cut = cut_of(half)
    raw_rows = min(cut, 160)
    width = wides[1]
    tile = 112 if half % 112 == 0 else 16
    n = wides[0] // width
    a, b = 1, (n + 1) // 2
    spans = [(0, 0, a), (0, a, b - a), (0, b, n - b)]
    parts = [[(which, c + i) for i in range(m)] for which, c, m in spans]
    parts[0].append((1, 0))
    parts[2].append((2, 0))
    batches = [(0, 1, 0, 1)] + [(i, *span) for i, span in enumerate(spans)] + [(2, 2, 0, 1)]
    pieces = [(1, 0, 1, 0, raw_rows, False), (*spans[0], 0, half, False)]
    pieces += [(1, 0, 1, raw_rows, cut - raw_rows, False), (1, 0, 1, cut, half - cut, True)]
    pieces += [(*span, 0, half, False) for span in spans[1:]] + [(2, 0, 1, 0, half, True)]
    piece = norm_train.shape[0]
    hbm = pl.BlockSpec(memory_space=pl.ANY)
    vmem = pl.BlockSpec(memory_space=pltpu.VMEM)
    dma = pltpu.SemaphoreType.DMA
    return pl.pallas_call(
        functools.partial(
            gather_kernel, count, across, width, half, tile, raw_rows, parts, batches, pieces
        ),
        in_specs=[hbm] * 8,
        out_specs=[vmem] * 10,
        out_shape=[pltpu.VMEM((count * rows, w), jnp.bfloat16) for w in wides]
        + [pltpu.VMEM((rows, w), jnp.float32) for w in wides]
        + [pltpu.VMEM((1, w), jnp.float32) for w in wides]
        + [pltpu.VMEM((count * across, 1, piece), jnp.float32)],
        scratch_shapes=[pltpu.VMEM(a.shape, jnp.float32) for a in arrays]
        + [
            pltpu.VMEM((1, piece), jnp.float32),
            pltpu.VMEM((1, piece), jnp.float32),
            pltpu.VMEM((count, 1, sum(wides)), jnp.float32),
            pltpu.VMEM((2, raw_rows, width), jnp.float32),
            dma((len(batches), 2)),
            dma((2,)),
            dma((1,)),
            dma((len(parts),)),
            dma((2,)),
            dma((2,)),
            dma((2,)),
            dma((2,)),
            dma((2, 2, len(pieces))),
            dma((2, 3, len(pieces))),
        ],
        compiler_params=pltpu.CompilerParams(
            collective_id=0, has_side_effects=True,
            vmem_limit_bytes=4 * sum(a.size for a in arrays) + 2**21,
        ),
    )(*arrays, norm_train.reshape(1, piece), norm_step.reshape(1, piece))


def pieces_of(source, target, sem, cuts):
    size = source.shape[0] // cuts
    copies = []
    for c in range(cuts):
        at = pl.ds(c * size, size)
        copies.append(pltpu.make_async_copy(source.at[at], target.at[at], sem.at[c]))
    return copies


def key_pieces(count, rows, late, small):
    half = rows // 2
    cut = cut_of(half)
    size = half - cut if late else cut
    pieces = []
    for owner in range(count):
        for way in range(2):
            spot = pl.ds(owner * rows + way * half + (cut if late else 0), size)
            pieces.append((pl.ds((owner * 2 + way) * size, size) if small else spot, spot))
    return pieces


def store_kernel(
    count, cuts,
    rk, rv, lq, lk, lv, scale_q, scale_k, scale_v, norm, rq,
    out_rk, out_rv, out_lq, out_lk, out_lv, out_sq, out_sk, out_sv, out_norm,
    sem, key_sem, own_sem,
):
    late = lax.rem(lax.axis_index("width"), 2) == 1
    rows = rv.shape[0] // count
    base = lax.axis_index("zero") * rows
    half = rows // 2
    cut = cut_of(half)
    both, last, first = [], [], []
    for i, (source, target) in enumerate(((lq, out_lq), (lk, out_lk), (lv, out_lv))):
        both += pieces_of(source, target, sem.at[i], cuts)
    first += pieces_of(rk, out_rk, sem.at[3], cuts) + pieces_of(rv, out_rv, sem.at[4], cuts)
    for i, (_, at) in enumerate(key_pieces(count, rows, False, False)):
        last.append(pltpu.make_async_copy(rk.at[at], out_rk.at[at], key_sem.at[i]))
    at = pl.ds(pl.multiple_of(base, 16), rows)
    last.append(pltpu.make_async_copy(rv.at[at], out_rv.at[at], own_sem.at[0]))
    for way in range(2):
        at = pl.ds(pl.multiple_of(base + way * half + cut, 16), half - cut)
        last.append(pltpu.make_async_copy(rk.at[at], out_rk.at[at], own_sem.at[1 + way]))

    for copy in both:
        copy.start()

    @pl.when(late)
    def _():
        for copy in last:
            copy.start()

    @pl.when(jnp.logical_not(late))
    def _():
        for copy in first:
            copy.start()

    for source, target in ((scale_q, out_sq), (scale_k, out_sk), (scale_v, out_sv)):
        target[...] = source[0, :]
    out_norm[...] = norm[...].astype(jnp.bfloat16)
    for copy in both:
        copy.wait()

    @pl.when(late)
    def _():
        for copy in last:
            copy.wait()

    @pl.when(jnp.logical_not(late))
    def _():
        for copy in first:
            copy.wait()


def store(arrays, count):
    cuts = 8
    dma = pltpu.SemaphoreType.DMA
    hbm = pl.BlockSpec(memory_space=pltpu.HBM)
    vmem = pl.BlockSpec(memory_space=pltpu.VMEM)
    return pl.pallas_call(
        functools.partial(store_kernel, count, cuts),
        in_specs=[vmem] * (len(arrays) - 1) + [hbm],
        out_specs=[hbm] * 5 + [vmem] * 4,
        out_shape=[jax.ShapeDtypeStruct(a.shape, a.dtype) for a in arrays[:5]]
        + [jax.ShapeDtypeStruct((a.shape[1],), a.dtype) for a in arrays[5:8]]
        + [jax.ShapeDtypeStruct(arrays[8].shape, jnp.bfloat16)],
        scratch_shapes=[dma((5, cuts)), dma((2 * count,)), dma((3,))],
        compiler_params=pltpu.CompilerParams(vmem_limit_bytes=2 * arrays[-1].size + 2**20),
    )(*arrays)


def store_one_kernel(cuts, source, target, sem):
    copies = pieces_of(source, target, sem, cuts)
    for copy in copies:
        copy.start()
    for copy in copies:
        copy.wait()


def store_one(array):
    cuts = 8
    return pl.pallas_call(
        functools.partial(store_one_kernel, cuts),
        in_specs=[pl.BlockSpec(memory_space=pltpu.VMEM)],
        out_specs=pl.BlockSpec(memory_space=pltpu.HBM),
        out_shape=jax.ShapeDtypeStruct(array.shape, array.dtype),
        scratch_shapes=[pltpu.SemaphoreType.DMA((cuts,))],
        compiler_params=pltpu.CompilerParams(vmem_limit_bytes=2**20),
    )(array)


def late_kernel(count, half, tile, own_k, own_v, after, rk, rv, load_sem, send_sem, recv_sem):
    me, node = ring_of(count)
    side = lax.axis_index("width")
    ahead, behind = node(1), node(-1)
    cut = cut_of(half)
    rest = half - cut
    pieces = [(rk, rest, t * tile) for t in range(rest // tile)]
    pieces += [(rv, half, t * tile) for t in range(half // tile)]

    def ring_copy(owner, step, p, way):
        ref, size, first = pieces[p]
        piece = ref.at[pl.ds(pl.multiple_of((owner * 2 + way) * size + first, 16), tile)]
        return pltpu.make_async_remote_copy(
            src_ref=piece, dst_ref=piece,
            send_sem=send_sem.at[way, lax.rem(step, 2), p], recv_sem=recv_sem.at[way, lax.rem(step, 3), p],
            device_id=(behind if way else ahead, side), device_id_type=MESH,
        )

    def owner_of(step, way):
        return node(step if way else -step)

    def leave(step):
        for p in range(len(pieces)):
            for way in range(2):
                ring_copy(owner_of(step, way), step, p, way).wait_send()

    @pl.when(lax.rem(side, 2) == 1)
    def _():
        barrier = pltpu.get_barrier_semaphore()
        for other in (ahead, behind):
            pl.semaphore_signal(barrier, inc=1, device_id=(other, side), device_id_type=MESH)
        loads = []
        for way in range(2):
            there = pl.ds(pl.multiple_of((me * 2 + way) * half + cut, 16), rest)
            here = pl.ds(pl.multiple_of((me * 2 + way) * rest, 16), rest)
            loads.append(pltpu.make_async_copy(own_k.at[there], rk.at[here], load_sem.at[0, way]))
            at = pl.ds(pl.multiple_of((me * 2 + way) * half, 16), half)
            loads.append(pltpu.make_async_copy(own_v.at[at], rv.at[at], load_sem.at[1, way]))
        for load in loads:
            load.start()
        for load in loads:
            load.wait()
        pl.semaphore_wait(barrier, 2)
        for p in range(len(pieces)):
            for way in range(2):
                ring_copy(me, 0, p, way).start()

        def forward(step, carry):
            for p in range(len(pieces)):
                for way in range(2):
                    ring_copy(owner_of(step, way), step - 1, p, way).wait_recv()
                    ring_copy(owner_of(step, way), step, p, way).start()
            leave(step - 1)
            return carry

        lax.fori_loop(1, count - 1, forward, 0)
        for p in range(len(pieces)):
            for way in range(2):
                ring_copy(owner_of(count - 1, way), count - 2, p, way).wait_recv()
        leave(count - 2)


def gather_late(own_k, own_v, after, count):
    half = own_k.shape[0] // count // 2
    rest = half - cut_of(half)
    tile = 112 if rest % 112 == 0 and half % 112 == 0 else 16
    n = (rest + half) // tile
    hbm = pl.BlockSpec(memory_space=pltpu.HBM)
    vmem = pl.BlockSpec(memory_space=pltpu.VMEM)
    dma = pltpu.SemaphoreType.DMA
    return pl.pallas_call(
        functools.partial(late_kernel, count, half, tile),
        in_specs=[hbm] * 3,
        out_specs=[vmem] * 2,
        out_shape=[
            pltpu.VMEM((2 * count * rest, own_k.shape[1]), own_k.dtype),
            pltpu.VMEM(own_v.shape, own_v.dtype),
        ],
        scratch_shapes=[dma((2, 2)), dma((2, 2, n)), dma((2, 3, n))],
        compiler_params=pltpu.CompilerParams(
            collective_id=1, has_side_effects=True, vmem_limit_bytes=56 * 2**20
        ),
    )(own_k, own_v, after)


def store_late_kernel(count, cuts, rk, rv, start_k, start_v, out_k, out_v, sem, key_sem):
    @pl.when(lax.rem(lax.axis_index("width"), 2) == 1)
    def _():
        copies = pieces_of(rv, out_v, sem, cuts)
        for copy in copies:
            copy.start()
        for here, there in key_pieces(count, rv.shape[0] // count, True, True):
            pltpu.make_async_copy(rk.at[here], out_k.at[there], key_sem).start()
        for copy in copies:
            copy.wait()
        pltpu.make_async_copy(rk, out_k.at[pl.ds(0, rk.shape[0])], key_sem).wait()


def store_late(rk, rv, start_k, start_v, count):
    cuts = 4
    hbm = pl.BlockSpec(memory_space=pltpu.HBM)
    vmem = pl.BlockSpec(memory_space=pltpu.VMEM)
    dma = pltpu.SemaphoreType.DMA
    return pl.pallas_call(
        functools.partial(store_late_kernel, count, cuts),
        in_specs=[vmem] * 2 + [hbm] * 2,
        out_specs=[hbm] * 2,
        out_shape=[jax.ShapeDtypeStruct(a.shape, a.dtype) for a in (start_k, start_v)],
        scratch_shapes=[dma((cuts,)), dma],
        input_output_aliases={2: 0, 3: 1},
        compiler_params=pltpu.CompilerParams(vmem_limit_bytes=40 * 2**20),
    )(rk, rv, start_k, start_v)


def solution(mesh):
    count, across = mesh.shape["zero"], mesh.shape["width"]

    def body(
        train_query, slow_query, train_key, slow_key, train_value, slow_value, norm_train, norm_step
    ):
        arrays = gather(
            (train_query, slow_query, train_key, slow_key, train_value, slow_value),
            norm_train, norm_step, count, across,
        )
        rq = store_one(arrays[0])
        rk, rv, lq, lk, lv, *scales, norm = store((*arrays[1:], rq), count)
        serve_norm = norm.reshape(-1)
        rk, rv = store_late(*gather_late(rk, rv, serve_norm, count), rk, rv, count)
        return (rq, rk, rv, *scales, serve_norm, lq, lk, lv)

    in_specs = (P("zero", "width"),) * 6 + (P(("zero", "width")),) * 2
    out_specs = (
        (P(None, "width"),) * 3 + (P("width"),) * 3 + (P(),) + (P("zero", "width"),) * 3
    )
    return jax.shard_map(body, mesh=mesh, in_specs=in_specs, out_specs=out_specs, check_vma=False)
```

```python
import functools

import jax
import jax.numpy as jnp
from jax import lax
from jax.experimental import pallas as pl
from jax.experimental.pallas import tpu as pltpu
from jax.sharding import PartitionSpec as P

keep_rate = 0.5
MESH = pl.DeviceIdType.MESH


def grid_of(count):
    fast = 1
    while (2 * fast) ** 2 <= count and count % (2 * fast) == 0:
        fast *= 2
    return count // fast, fast


def node_at(place, slow, fast):
    if fast == 1:
        return place
    deep = slow - 1
    back = place // (deep * fast)
    column = place // deep
    step = place % deep
    step = step + (column % 2) * (deep - 1 - 2 * step)
    z = (1 - back) * (1 + step)
    y = (1 - back) * column + back * (fast - 1 - (place - deep * fast))
    return z * fast + y


def place_of(node, slow, fast):
    if fast == 1:
        return node
    deep = slow - 1
    z, y = node // fast, node % fast
    out = (z + slow - 1) // slow
    step = z - 1
    step = step + (y % 2) * (deep - 1 - 2 * step)
    return out * (y * deep + step) + (1 - out) * (deep * fast + fast - 1 - y)


def ring_of(count):
    me = lax.axis_index("zero")
    slow, fast = grid_of(count)
    place = place_of(me, slow, fast)

    def node(step):
        return node_at(lax.rem(place + count + step, count), slow, fast)

    return me, node


def gather_kernel(
    count, across, width, half, tile, raw_rows, parts, batches, pieces,
    tq, sq, tk, sk, tv, sv, norm_train, norm_step,
    rq, rk, rv, lq, lk, lv, scale_q, scale_k, scale_v, norm_all,
    itq, isq, itk, isk, itv, isv, in_train, in_step, stats, raw,
    load_sem, norm_sem, stat_send, stat_recv, near_sem, far_sem, raw_send, raw_recv,
    send_sem, recv_sem,
):
    me, node = ring_of(count)
    side = lax.axis_index("width")
    late = lax.rem(side, 2) == 1
    ahead, behind = node(1), node(-1)
    rows = 2 * half
    trains, slows = ((tq, itq), (tk, itk), (tv, itv)), ((sq, isq), (sk, isk), (sv, isv))
    latest, ready, scales = (lq, lk, lv), (rq, rk, rv), (scale_q, scale_k, scale_v)
    groups = [group for part in parts for group in part]

    def columns(c, n=1):
        return pl.ds(c * width, n * width)

    def allowed(p, action):
        if pieces[p][5]:
            pl.when(jnp.logical_not(late))(action)
        else:
            action()

    barrier = pltpu.get_barrier_semaphore()
    for k in range(1, count):
        pl.semaphore_signal(
            barrier, inc=1, device_id=(lax.rem(me + k, count), side), device_id_type=MESH
        )
    for k in range(1, across):
        pl.semaphore_signal(
            barrier, inc=1, device_id=(me, lax.rem(side + k, across)), device_id_type=MESH
        )

    loads = []
    for i, (_, which, c, n) in enumerate(batches):
        for j, arrays in enumerate((trains, slows)):
            far, near = arrays[which]
            loads.append(
                pltpu.make_async_copy(
                    far.at[:, columns(c, n)], near.at[:, columns(c, n)], load_sem.at[i, j]
                )
            )
            loads[-1].start()
    norms = [
        pltpu.make_async_copy(far, near, norm_sem.at[j])
        for j, (far, near) in enumerate(((norm_train, in_train), (norm_step, in_step)))
    ]
    for load in norms:
        load.start()
    mine = me * across + side

    def part_columns(part):
        first = groups.index(parts[part][0])
        return columns(first, len(parts[part]))

    def stat_copy(part, k):
        piece = stats.at[me, :, part_columns(part)]
        return pltpu.make_async_remote_copy(
            src_ref=piece, dst_ref=piece, send_sem=stat_send.at[0], recv_sem=stat_recv.at[part],
            device_id=(lax.rem(me + k, count), side), device_id_type=MESH,
        )

    def all_stats(part=None):
        piece = stats.at[pl.ds(0, count - 1)]
        if part is not None:
            piece = stats.at[pl.ds(0, count - 1), :, part_columns(part)]
        return pltpu.make_async_remote_copy(
            src_ref=piece, dst_ref=piece, send_sem=stat_send.at[0],
            recv_sem=stat_recv.at[part or 0], device_id=(ahead, side), device_id_type=MESH,
        )

    def near_copy(at, k=1):
        return pltpu.make_async_remote_copy(
            src_ref=norm_all.at[at], dst_ref=norm_all.at[at],
            send_sem=near_sem.at[0], recv_sem=near_sem.at[1],
            device_id=(me, lax.rem(side + k, across)), device_id_type=MESH,
        )

    def far_copy(at, k=1):
        return pltpu.make_async_remote_copy(
            src_ref=norm_all.at[at], dst_ref=norm_all.at[at],
            send_sem=far_sem.at[0], recv_sem=far_sem.at[1],
            device_id=(lax.rem(me + k, count), side), device_id_type=MESH,
        )

    all_near = near_copy(pl.ds(0, across - 1))
    all_far = far_copy(pl.ds(0, (count - 1) * across))

    def average(i):
        which, c = groups[i]

        def step(t, total):
            at = pl.ds(pl.multiple_of(t * tile, 16), tile)
            value = (
                keep_rate * slows[which][1][at, columns(c)]
                + (1.0 - keep_rate) * trains[which][1][at, columns(c)]
            )
            latest[which][at, columns(c)] = value
            return total + jnp.sum((value * value).reshape(tile // 8, 8, width), axis=0)

        total = lax.fori_loop(0, rows // tile, step, jnp.zeros((8, width), jnp.float32))
        stats[me, :, columns(i)] = jnp.sum(total, axis=0, keepdims=True)

    def averages(part):
        for i, batch in enumerate(batches):
            if batch[0] == part:
                loads[2 * i].wait()
                loads[2 * i + 1].wait()
        for group in parts[part]:
            average(groups.index(group))

    def ring_copy(owner, step, p, way):
        which, c, n, first, size, _ = pieces[p]
        spot = pl.ds(pl.multiple_of(owner * rows + way * half + first, 16), size)
        piece = ready[which].at[spot, columns(c, n)]
        return pltpu.make_async_remote_copy(
            src_ref=piece, dst_ref=piece,
            send_sem=send_sem.at[way, lax.rem(step, 2)],
            recv_sem=recv_sem.at[way, lax.rem(step, 3), p],
            device_id=(behind if way else ahead, side), device_id_type=MESH,
        )

    def raw_copy(way):
        return pltpu.make_async_remote_copy(
            src_ref=lk.at[pl.ds(way * half, raw_rows)], dst_ref=raw.at[way],
            send_sem=raw_send.at[way], recv_sem=raw_recv.at[way],
            device_id=(behind if way else ahead, side), device_id_type=MESH,
        )

    def owner_of(step, way):
        return node(step if way else -step)

    def send_own(part):
        for p, (which, c, n, first, size, _) in enumerate(pieces):
            if (which, c) not in parts[part]:
                continue
            for way in range(2):
                for each in range(c, c + n):
                    scale = scales[which][:, columns(each)]
                    short = tile if size % tile == 0 else 16

                    def step(t, carry):
                        at = pl.multiple_of(way * half + first + t * short, 16)
                        home = pl.multiple_of(me * rows + at, 16)
                        ready[which][pl.ds(home, short), columns(each)] = (
                            latest[which][pl.ds(at, short), columns(each)] / scale
                        ).astype(jnp.bfloat16)
                        return carry

                    lax.fori_loop(0, size // short, step, 0)
                if p:
                    allowed(p, lambda: ring_copy(me, 0, p, way).start())

    def tell(part):
        for k in range(1, count):
            stat_copy(part, k).start()

    def finish(part):
        all_stats(part).wait_recv()
        for group in parts[part]:
            i = groups.index(group)
            which, c = group
            total = stats[0, :, columns(i)]
            for k in range(1, count):
                total = total + stats[k, :, columns(i)]
            scales[which][:, columns(c)] = jnp.sqrt(total)

    for part in range(len(parts)):
        averages(part)
        if part == 0:
            pl.semaphore_wait(barrier, count + across - 2)
        tell(part)
        if part == 0:
            for way in range(2):
                raw_copy(way).start()
            for load in norms:
                load.wait()
            norm_all[mine] = in_train[...] + in_step[...]
            for k in range(1, across):
                near_copy(mine, k).start()
        else:
            finish(part - 1)
            send_own(part - 1)
    finish(len(parts) - 1)
    send_own(len(parts) - 1)
    all_near.wait_recv()
    for k in range(1, count):
        far_copy(pl.ds(me * across, across), k).start()

    def leave(step):
        def left(n):
            whole = rk.at[pl.ds(0, n)]
            for way in range(2):
                pltpu.make_async_remote_copy(
                    src_ref=whole, dst_ref=whole, send_sem=send_sem.at[way, lax.rem(step, 2)],
                    recv_sem=recv_sem.at[way, 0, 0], device_id=(ahead, side), device_id_type=MESH,
                ).wait_send()

        for kind in (late, jnp.logical_not(late)):
            n = sum(p[2] * p[4] for p in pieces if kind is not late or not p[5])
            pl.when(jnp.logical_and(kind, step > 0))(functools.partial(left, n))
            pl.when(jnp.logical_and(kind, step == 0))(functools.partial(left, n - raw_rows))

    def pass_raw():
        short = tile if raw_rows % tile == 0 else 16
        for way in range(2):
            raw_copy(way).wait_recv()
            home = owner_of(1, way) * rows + way * half

            def step(t, carry):
                at = pl.ds(pl.multiple_of(t * short, 16), short)
                rk[pl.ds(pl.multiple_of(home + t * short, 16), short), :] = (
                    raw[way, at, :] / scale_k[...]
                ).astype(jnp.bfloat16)
                return carry

            lax.fori_loop(0, raw_rows // short, step, 0)
            ring_copy(owner_of(1, way), 1, 0, way).start()

    def forward(step, carry):
        owners = owner_of(step, 0), owner_of(step, 1)
        for p in range(len(pieces)):

            def pass_on():
                for way in range(2):
                    ring_copy(owners[way], step - 1, p, way).wait_recv()
                    ring_copy(owners[way], step, p, way).start()

            if p:
                allowed(p, pass_on)
            else:
                pl.when(step > 1)(pass_on)
        leave(step - 1)
        return carry

    pass_raw()
    lax.fori_loop(1, count - 1, forward, 0)
    for way in range(2):
        raw_copy(way).wait_send()
    all_stats().wait_send()
    all_near.wait_send()
    all_far.wait_send()
    all_far.wait_recv()
    for p in range(len(pieces)):

        def arrive():
            for way in range(2):
                ring_copy(owner_of(count - 1, way), count - 2, p, way).wait_recv()

        allowed(p, arrive)
    leave(count - 2)


def cut_of(half):
    return half // 4 * 3


def gather(arrays, norm_train, norm_step, count, across):
    rows = arrays[0].shape[0]
    wides = [a.shape[1] for a in arrays[::2]]
    half = rows // 2
    cut = cut_of(half)
    raw_rows = min(cut, 160)
    width = wides[1]
    tile = 112 if half % 112 == 0 else 16
    n = wides[0] // width
    a, b = 1, (n + 1) // 2
    spans = [(0, 0, a), (0, a, b - a), (0, b, n - b)]
    parts = [[(which, c + i) for i in range(m)] for which, c, m in spans]
    parts[0].append((1, 0))
    parts[2].append((2, 0))
    batches = [(0, 1, 0, 1)] + [(i, *span) for i, span in enumerate(spans)] + [(2, 2, 0, 1)]
    pieces = [(1, 0, 1, 0, raw_rows, False), (*spans[0], 0, half, False)]
    pieces += [(1, 0, 1, raw_rows, cut - raw_rows, False), (1, 0, 1, cut, half - cut, True)]
    pieces += [(*span, 0, half, False) for span in spans[1:]] + [(2, 0, 1, 0, half, True)]
    piece = norm_train.shape[0]
    hbm = pl.BlockSpec(memory_space=pl.ANY)
    vmem = pl.BlockSpec(memory_space=pltpu.VMEM)
    dma = pltpu.SemaphoreType.DMA
    return pl.pallas_call(
        functools.partial(
            gather_kernel, count, across, width, half, tile, raw_rows, parts, batches, pieces
        ),
        in_specs=[hbm] * 8,
        out_specs=[vmem] * 10,
        out_shape=[pltpu.VMEM((count * rows, w), jnp.bfloat16) for w in wides]
        + [pltpu.VMEM((rows, w), jnp.float32) for w in wides]
        + [pltpu.VMEM((1, w), jnp.float32) for w in wides]
        + [pltpu.VMEM((count * across, 1, piece), jnp.float32)],
        scratch_shapes=[pltpu.VMEM(a.shape, jnp.float32) for a in arrays]
        + [
            pltpu.VMEM((1, piece), jnp.float32),
            pltpu.VMEM((1, piece), jnp.float32),
            pltpu.VMEM((count, 1, sum(wides)), jnp.float32),
            pltpu.VMEM((2, raw_rows, width), jnp.float32),
            dma((len(batches), 2)),
            dma((2,)),
            dma((1,)),
            dma((len(parts),)),
            dma((2,)),
            dma((2,)),
            dma((2,)),
            dma((2,)),
            dma((2, 2)),
            dma((2, 3, len(pieces))),
        ],
        compiler_params=pltpu.CompilerParams(
            collective_id=0, has_side_effects=True,
            vmem_limit_bytes=4 * sum(a.size for a in arrays) + 2**21,
        ),
    )(*arrays, norm_train.reshape(1, piece), norm_step.reshape(1, piece))


def pieces_of(source, target, sem, cuts):
    size = source.shape[0] // cuts
    copies = []
    for c in range(cuts):
        at = pl.ds(c * size, size)
        copies.append(pltpu.make_async_copy(source.at[at], target.at[at], sem.at[c]))
    return copies


def early_key(count, rows):
    half = rows // 2
    return [pl.ds(i * half, cut_of(half)) for i in range(2 * count)]


def store_kernel(
    count, cuts,
    rk, rv, lq, lk, lv, scale_q, scale_k, scale_v, norm, rq,
    out_rk, out_rv, out_lq, out_lk, out_lv, out_sq, out_sk, out_sv, out_norm,
    sem, key_sem, own_sem,
):
    late = lax.rem(lax.axis_index("width"), 2) == 1
    rows = rv.shape[0] // count
    base = lax.axis_index("zero") * rows
    half = rows // 2
    cut = cut_of(half)
    both, last, first = [], [], []
    for i, (source, target) in enumerate(((lq, out_lq), (lk, out_lk), (lv, out_lv))):
        both += pieces_of(source, target, sem.at[i], cuts)
    first += pieces_of(rk, out_rk, sem.at[3], cuts) + pieces_of(rv, out_rv, sem.at[4], cuts)
    for i, at in enumerate(early_key(count, rows)):
        last.append(pltpu.make_async_copy(rk.at[at], out_rk.at[at], key_sem.at[i]))
    at = pl.ds(pl.multiple_of(base, 16), rows)
    last.append(pltpu.make_async_copy(rv.at[at], out_rv.at[at], own_sem.at[0]))
    for way in range(2):
        at = pl.ds(pl.multiple_of(base + way * half + cut, 16), half - cut)
        last.append(pltpu.make_async_copy(rk.at[at], out_rk.at[at], own_sem.at[1 + way]))

    for copy in both:
        copy.start()

    @pl.when(late)
    def _():
        for copy in last:
            copy.start()

    @pl.when(jnp.logical_not(late))
    def _():
        for copy in first:
            copy.start()

    for source, target in ((scale_q, out_sq), (scale_k, out_sk), (scale_v, out_sv)):
        target[...] = source[0, :]
    out_norm[...] = norm[...].astype(jnp.bfloat16)
    for copy in both:
        copy.wait()

    @pl.when(late)
    def _():
        for copy in last:
            copy.wait()

    @pl.when(jnp.logical_not(late))
    def _():
        for copy in first:
            copy.wait()


def store(arrays, count):
    cuts = 8
    dma = pltpu.SemaphoreType.DMA
    hbm = pl.BlockSpec(memory_space=pltpu.HBM)
    vmem = pl.BlockSpec(memory_space=pltpu.VMEM)
    return pl.pallas_call(
        functools.partial(store_kernel, count, cuts),
        in_specs=[vmem] * (len(arrays) - 1) + [hbm],
        out_specs=[hbm] * 5 + [vmem] * 4,
        out_shape=[jax.ShapeDtypeStruct(a.shape, a.dtype) for a in arrays[:5]]
        + [jax.ShapeDtypeStruct((a.shape[1],), a.dtype) for a in arrays[5:8]]
        + [jax.ShapeDtypeStruct(arrays[8].shape, jnp.bfloat16)],
        scratch_shapes=[dma((5, cuts)), dma((2 * count,)), dma((3,))],
        compiler_params=pltpu.CompilerParams(vmem_limit_bytes=2 * arrays[-1].size + 2**20),
    )(*arrays)


def store_one_kernel(cuts, source, target, sem):
    copies = pieces_of(source, target, sem, cuts)
    for copy in copies:
        copy.start()
    for copy in copies:
        copy.wait()


def store_one(array):
    cuts = 8
    return pl.pallas_call(
        functools.partial(store_one_kernel, cuts),
        in_specs=[pl.BlockSpec(memory_space=pltpu.VMEM)],
        out_specs=pl.BlockSpec(memory_space=pltpu.HBM),
        out_shape=jax.ShapeDtypeStruct(array.shape, array.dtype),
        scratch_shapes=[pltpu.SemaphoreType.DMA((cuts,))],
        compiler_params=pltpu.CompilerParams(vmem_limit_bytes=2**20),
    )(array)


def late_kernel(count, half, tile, own_k, own_v, after, rk, rv, load_sem, send_sem, recv_sem):
    me, node = ring_of(count)
    side = lax.axis_index("width")
    ahead, behind = node(1), node(-1)
    cut = cut_of(half)
    rest = half - cut
    pieces = [(rk, rest, t * tile) for t in range(rest // tile)]
    pieces += [(rv, half, t * tile) for t in range(half // tile)]

    def ring_copy(owner, step, p, way):
        ref, size, first = pieces[p]
        piece = ref.at[pl.ds(pl.multiple_of((owner * 2 + way) * size + first, 16), tile)]
        return pltpu.make_async_remote_copy(
            src_ref=piece, dst_ref=piece,
            send_sem=send_sem.at[way, lax.rem(step, 2)], recv_sem=recv_sem.at[way, lax.rem(step, 3), p],
            device_id=(behind if way else ahead, side), device_id_type=MESH,
        )

    def owner_of(step, way):
        return node(step if way else -step)

    def leave(step):
        whole = rv.at[pl.ds(0, rest + half)]
        for way in range(2):
            pltpu.make_async_remote_copy(
                src_ref=whole, dst_ref=whole, send_sem=send_sem.at[way, lax.rem(step, 2)],
                recv_sem=recv_sem.at[way, 0, 0], device_id=(ahead, side), device_id_type=MESH,
            ).wait_send()

    @pl.when(lax.rem(side, 2) == 1)
    def _():
        barrier = pltpu.get_barrier_semaphore()
        for other in (ahead, behind):
            pl.semaphore_signal(barrier, inc=1, device_id=(other, side), device_id_type=MESH)
        loads = []
        for way in range(2):
            there = pl.ds(pl.multiple_of((me * 2 + way) * half + cut, 16), rest)
            here = pl.ds(pl.multiple_of((me * 2 + way) * rest, 16), rest)
            loads.append(pltpu.make_async_copy(own_k.at[there], rk.at[here], load_sem.at[0, way]))
            at = pl.ds(pl.multiple_of((me * 2 + way) * half, 16), half)
            loads.append(pltpu.make_async_copy(own_v.at[at], rv.at[at], load_sem.at[1, way]))
        for load in loads:
            load.start()
        for load in loads:
            load.wait()
        pl.semaphore_wait(barrier, 2)
        for p in range(len(pieces)):
            for way in range(2):
                ring_copy(me, 0, p, way).start()

        def forward(step, carry):
            for p in range(len(pieces)):
                for way in range(2):
                    ring_copy(owner_of(step, way), step - 1, p, way).wait_recv()
                    ring_copy(owner_of(step, way), step, p, way).start()
            leave(step - 1)
            return carry

        lax.fori_loop(1, count - 1, forward, 0)
        for p in range(len(pieces)):
            for way in range(2):
                ring_copy(owner_of(count - 1, way), count - 2, p, way).wait_recv()
        leave(count - 2)


def gather_late(own_k, own_v, after, count):
    half = own_k.shape[0] // count // 2
    rest = half - cut_of(half)
    tile = 112 if rest % 112 == 0 and half % 112 == 0 else 16
    n = (rest + half) // tile
    hbm = pl.BlockSpec(memory_space=pltpu.HBM)
    vmem = pl.BlockSpec(memory_space=pltpu.VMEM)
    dma = pltpu.SemaphoreType.DMA
    return pl.pallas_call(
        functools.partial(late_kernel, count, half, tile),
        in_specs=[hbm] * 3,
        out_specs=[vmem] * 2,
        out_shape=[
            pltpu.VMEM((2 * count * rest, own_k.shape[1]), own_k.dtype),
            pltpu.VMEM(own_v.shape, own_v.dtype),
        ],
        scratch_shapes=[dma((2, 2)), dma((2, 2)), dma((2, 3, n))],
        compiler_params=pltpu.CompilerParams(
            collective_id=1, has_side_effects=True, vmem_limit_bytes=56 * 2**20
        ),
    )(own_k, own_v, after)


def store_late_kernel(count, rk, rv, start_k, start_v, out_k, out_v, sem):
    me, side = lax.axis_index("zero"), lax.axis_index("width")
    rows, rest = rv.shape[0] // count, rk.shape[0] // count // 2
    half = rows // 2

    @pl.when(lax.rem(side, 2) == 1)
    def _():
        for k in range(1, count):
            owner = lax.rem(me + k, count)
            at = pl.ds(pl.multiple_of(owner * rows, 16), rows)
            pltpu.make_async_copy(rv.at[at], out_v.at[at], sem.at[0]).start()
            for way in range(2):
                here = pl.ds(pl.multiple_of((owner * 2 + way) * rest, 16), rest)
                there = pl.ds(pl.multiple_of(owner * rows + way * half + half - rest, 16), rest)
                pltpu.make_async_copy(rk.at[here], out_k.at[there], sem.at[1]).start()
        for i, (near, far) in enumerate(((rv, out_v), (rk, out_k))):
            n = near.shape[0] // count * (count - 1)
            pltpu.make_async_copy(near.at[pl.ds(0, n)], far.at[pl.ds(0, n)], sem.at[i]).wait()


def store_late(rk, rv, start_k, start_v, count):
    hbm = pl.BlockSpec(memory_space=pltpu.HBM)
    vmem = pl.BlockSpec(memory_space=pltpu.VMEM)
    dma = pltpu.SemaphoreType.DMA
    return pl.pallas_call(
        functools.partial(store_late_kernel, count),
        in_specs=[vmem] * 2 + [hbm] * 2,
        out_specs=[hbm] * 2,
        out_shape=[jax.ShapeDtypeStruct(a.shape, a.dtype) for a in (start_k, start_v)],
        scratch_shapes=[dma((2,))],
        input_output_aliases={2: 0, 3: 1},
        compiler_params=pltpu.CompilerParams(vmem_limit_bytes=40 * 2**20),
    )(rk, rv, start_k, start_v)


def solution(mesh):
    count, across = mesh.shape["zero"], mesh.shape["width"]

    def body(
        train_query, slow_query, train_key, slow_key, train_value, slow_value, norm_train, norm_step
    ):
        arrays = gather(
            (train_query, slow_query, train_key, slow_key, train_value, slow_value),
            norm_train, norm_step, count, across,
        )
        rq = store_one(arrays[0])
        rk, rv, lq, lk, lv, *scales, norm = store((*arrays[1:], rq), count)
        serve_norm = norm.reshape(-1)
        rk, rv = store_late(*gather_late(rk, rv, serve_norm, count), rk, rv, count)
        return (rq, rk, rv, *scales, serve_norm, lq, lk, lv)

    in_specs = (P("zero", "width"),) * 6 + (P(("zero", "width")),) * 2
    out_specs = (
        (P(None, "width"),) * 3 + (P("width"),) * 3 + (P(),) + (P("zero", "width"),) * 3
    )
    return jax.shard_map(body, mesh=mesh, in_specs=in_specs, out_specs=out_specs, check_vma=False)
```

```python
import functools

import jax
import jax.numpy as jnp
from jax import lax
from jax.experimental import pallas as pl
from jax.experimental.pallas import tpu as pltpu
from jax.sharding import PartitionSpec as P

keep_rate = 0.5
MESH = pl.DeviceIdType.MESH


def grid_of(count):
    fast = 1
    while (2 * fast) ** 2 <= count and count % (2 * fast) == 0:
        fast *= 2
    return count // fast, fast


def node_at(place, slow, fast):
    if fast == 1:
        return place
    deep = slow - 1
    back = place // (deep * fast)
    column = place // deep
    step = place % deep
    step = step + (column % 2) * (deep - 1 - 2 * step)
    z = (1 - back) * (1 + step)
    y = (1 - back) * column + back * (fast - 1 - (place - deep * fast))
    return z * fast + y


def place_of(node, slow, fast):
    if fast == 1:
        return node
    deep = slow - 1
    z, y = node // fast, node % fast
    out = (z + slow - 1) // slow
    step = z - 1
    step = step + (y % 2) * (deep - 1 - 2 * step)
    return out * (y * deep + step) + (1 - out) * (deep * fast + fast - 1 - y)


def ring_of(count):
    me = lax.axis_index("zero")
    slow, fast = grid_of(count)
    place = place_of(me, slow, fast)

    def node(step):
        return node_at(lax.rem(place + count + step, count), slow, fast)

    return me, node


def gather_kernel(
    count, across, width, half, tile, raw_rows, parts, batches, pieces,
    tq, sq, tk, sk, tv, sv, norm_train, norm_step,
    rq, rk, rv, lq, lk, lv, scale_q, scale_k, scale_v, norm_all,
    itq, isq, itk, isk, itv, isv, in_train, in_step, stats, raw,
    load_sem, norm_sem, stat_send, stat_recv, near_sem, far_sem, raw_send, raw_recv,
    send_sem, recv_sem,
):
    me, node = ring_of(count)
    side = lax.axis_index("width")
    late = lax.rem(side, 2) == 1
    ahead, behind = node(1), node(-1)
    rows = 2 * half
    trains, slows = ((tq, itq), (tk, itk), (tv, itv)), ((sq, isq), (sk, isk), (sv, isv))
    latest, ready, scales = (lq, lk, lv), (rq, rk, rv), (scale_q, scale_k, scale_v)
    groups = [group for part in parts for group in part]

    def columns(c, n=1):
        return pl.ds(c * width, n * width)

    def allowed(p, action):
        if pieces[p][5]:
            pl.when(jnp.logical_not(late))(action)
        else:
            action()

    barrier = pltpu.get_barrier_semaphore()
    for k in range(1, count):
        pl.semaphore_signal(
            barrier, inc=1, device_id=(lax.rem(me + k, count), side), device_id_type=MESH
        )
    for k in range(1, across):
        pl.semaphore_signal(
            barrier, inc=1, device_id=(me, lax.rem(side + k, across)), device_id_type=MESH
        )

    loads = []
    for i, (_, which, c, n) in enumerate(batches):
        for j, arrays in enumerate((trains, slows)):
            far, near = arrays[which]
            loads.append(
                pltpu.make_async_copy(
                    far.at[:, columns(c, n)], near.at[:, columns(c, n)], load_sem.at[i, j]
                )
            )
            loads[-1].start()
    norms = [
        pltpu.make_async_copy(far, near, norm_sem.at[j])
        for j, (far, near) in enumerate(((norm_train, in_train), (norm_step, in_step)))
    ]
    for load in norms:
        load.start()
    mine = me * across + side

    def part_columns(part):
        first = groups.index(parts[part][0])
        return columns(first, len(parts[part]))

    def stat_copy(part, k):
        piece = stats.at[me, :, part_columns(part)]
        return pltpu.make_async_remote_copy(
            src_ref=piece, dst_ref=piece, send_sem=stat_send.at[0], recv_sem=stat_recv.at[part],
            device_id=(lax.rem(me + k, count), side), device_id_type=MESH,
        )

    def all_stats(part=None):
        piece = stats.at[pl.ds(0, count - 1)]
        if part is not None:
            piece = stats.at[pl.ds(0, count - 1), :, part_columns(part)]
        return pltpu.make_async_remote_copy(
            src_ref=piece, dst_ref=piece, send_sem=stat_send.at[0],
            recv_sem=stat_recv.at[part or 0], device_id=(ahead, side), device_id_type=MESH,
        )

    def near_copy(at, k=1):
        return pltpu.make_async_remote_copy(
            src_ref=norm_all.at[at], dst_ref=norm_all.at[at],
            send_sem=near_sem.at[0], recv_sem=near_sem.at[1],
            device_id=(me, lax.rem(side + k, across)), device_id_type=MESH,
        )

    def far_copy(at, k=1):
        return pltpu.make_async_remote_copy(
            src_ref=norm_all.at[at], dst_ref=norm_all.at[at],
            send_sem=far_sem.at[0], recv_sem=far_sem.at[1],
            device_id=(lax.rem(me + k, count), side), device_id_type=MESH,
        )

    all_near = near_copy(pl.ds(0, across - 1))
    all_far = far_copy(pl.ds(0, (count - 1) * across))

    def average(i):
        which, c = groups[i]

        def step(t, total):
            at = pl.ds(pl.multiple_of(t * tile, 16), tile)
            value = (
                keep_rate * slows[which][1][at, columns(c)]
                + (1.0 - keep_rate) * trains[which][1][at, columns(c)]
            )
            latest[which][at, columns(c)] = value
            return total + jnp.sum((value * value).reshape(tile // 8, 8, width), axis=0)

        total = lax.fori_loop(0, rows // tile, step, jnp.zeros((8, width), jnp.float32))
        stats[me, :, columns(i)] = jnp.sum(total, axis=0, keepdims=True)

    def averages(part):
        for i, batch in enumerate(batches):
            if batch[0] == part:
                loads[2 * i].wait()
                loads[2 * i + 1].wait()
        for group in parts[part]:
            average(groups.index(group))

    def ring_copy(owner, step, p, way):
        which, c, n, first, size, _ = pieces[p]
        spot = pl.ds(pl.multiple_of(owner * rows + way * half + first, 16), size)
        piece = ready[which].at[spot, columns(c, n)]
        return pltpu.make_async_remote_copy(
            src_ref=piece, dst_ref=piece,
            send_sem=send_sem.at[way, lax.rem(step, 2)],
            recv_sem=recv_sem.at[way, lax.rem(step, 3), p],
            device_id=(behind if way else ahead, side), device_id_type=MESH,
        )

    def raw_copy(way):
        return pltpu.make_async_remote_copy(
            src_ref=lk.at[pl.ds(way * half, raw_rows)], dst_ref=raw.at[way],
            send_sem=raw_send.at[way], recv_sem=raw_recv.at[way],
            device_id=(behind if way else ahead, side), device_id_type=MESH,
        )

    def owner_of(step, way):
        return node(step if way else -step)

    def send_own(part):
        for p, (which, c, n, first, size, _) in enumerate(pieces):
            if (which, c) not in parts[part]:
                continue
            for way in range(2):
                for each in range(c, c + n):
                    scale = scales[which][:, columns(each)]
                    short = tile if size % tile == 0 else 16

                    def step(t, carry):
                        at = pl.multiple_of(way * half + first + t * short, 16)
                        home = pl.multiple_of(me * rows + at, 16)
                        ready[which][pl.ds(home, short), columns(each)] = (
                            latest[which][pl.ds(at, short), columns(each)] / scale
                        ).astype(jnp.bfloat16)
                        return carry

                    lax.fori_loop(0, size // short, step, 0)
                if p:
                    allowed(p, lambda: ring_copy(me, 0, p, way).start())

    def tell(part):
        for k in range(1, count):
            stat_copy(part, k).start()

    def finish(part):
        all_stats(part).wait_recv()
        for group in parts[part]:
            i = groups.index(group)
            which, c = group
            total = stats[0, :, columns(i)]
            for k in range(1, count):
                total = total + stats[k, :, columns(i)]
            scales[which][:, columns(c)] = jnp.sqrt(total)

    for part in range(len(parts)):
        averages(part)
        if part == 0:
            pl.semaphore_wait(barrier, count + across - 2)
        tell(part)
        if part == 0:
            for way in range(2):
                raw_copy(way).start()
            for load in norms:
                load.wait()
            norm_all[mine] = in_train[...] + in_step[...]
            for k in range(1, across):
                near_copy(mine, k).start()
        else:
            finish(part - 1)
            send_own(part - 1)
    finish(len(parts) - 1)
    send_own(len(parts) - 1)
    all_near.wait_recv()
    for k in range(1, count):
        far_copy(pl.ds(me * across, across), k).start()

    def leave(step):
        def left(n):
            whole = rk.at[pl.ds(0, n)]
            for way in range(2):
                pltpu.make_async_remote_copy(
                    src_ref=whole, dst_ref=whole, send_sem=send_sem.at[way, lax.rem(step, 2)],
                    recv_sem=recv_sem.at[way, 0, 0], device_id=(ahead, side), device_id_type=MESH,
                ).wait_send()

        for kind in (late, jnp.logical_not(late)):
            n = sum(p[2] * p[4] for p in pieces if kind is not late or not p[5])
            pl.when(jnp.logical_and(kind, step > 0))(functools.partial(left, n))
            pl.when(jnp.logical_and(kind, step == 0))(functools.partial(left, n - raw_rows))

    def pass_raw():
        short = tile if raw_rows % tile == 0 else 16
        for way in range(2):
            raw_copy(way).wait_recv()
            home = owner_of(1, way) * rows + way * half

            def step(t, carry):
                at = pl.ds(pl.multiple_of(t * short, 16), short)
                rk[pl.ds(pl.multiple_of(home + t * short, 16), short), :] = (
                    raw[way, at, :] / scale_k[...]
                ).astype(jnp.bfloat16)
                return carry

            lax.fori_loop(0, raw_rows // short, step, 0)
            ring_copy(owner_of(1, way), 1, 0, way).start()

    def forward(step, carry):
        owners = owner_of(step, 0), owner_of(step, 1)
        for p in range(len(pieces)):

            def pass_on():
                for way in range(2):
                    ring_copy(owners[way], step - 1, p, way).wait_recv()
                    ring_copy(owners[way], step, p, way).start()

            if p:
                allowed(p, pass_on)
            else:
                pl.when(step > 1)(pass_on)
        leave(step - 1)
        return carry

    pass_raw()
    lax.fori_loop(1, count - 1, forward, 0)
    for way in range(2):
        raw_copy(way).wait_send()
    all_stats().wait_send()
    all_near.wait_send()
    all_far.wait_send()
    all_far.wait_recv()
    for p in range(len(pieces)):

        def arrive():
            for way in range(2):
                ring_copy(owner_of(count - 1, way), count - 2, p, way).wait_recv()

        allowed(p, arrive)
    leave(count - 2)


def cut_of(half):
    return half - (112 if half % 112 == 0 and half > 112 else half // 64 * 16)


def gather(arrays, norm_train, norm_step, count, across):
    rows = arrays[0].shape[0]
    wides = [a.shape[1] for a in arrays[::2]]
    half = rows // 2
    cut = cut_of(half)
    raw_rows = cut // 32 * 16
    width = wides[1]
    tile = 112 if half % 112 == 0 else 16
    n = wides[0] // width
    a, b = 1, (n + 1) // 2
    spans = [(0, 0, a), (0, a, b - a), (0, b, n - b)]
    parts = [[(which, c + i) for i in range(m)] for which, c, m in spans]
    parts[0].append((1, 0))
    parts[2].append((2, 0))
    batches = [(0, 1, 0, 1)] + [(i, *span) for i, span in enumerate(spans)] + [(2, 2, 0, 1)]
    pieces = [(1, 0, 1, 0, raw_rows, False), (*spans[0], 0, half, False)]
    pieces += [(1, 0, 1, raw_rows, cut - raw_rows, False), (1, 0, 1, cut, half - cut, True)]
    pieces += [(*span, 0, half, False) for span in spans[1:]] + [(2, 0, 1, 0, half, True)]
    piece = norm_train.shape[0]
    hbm = pl.BlockSpec(memory_space=pl.ANY)
    vmem = pl.BlockSpec(memory_space=pltpu.VMEM)
    dma = pltpu.SemaphoreType.DMA
    return pl.pallas_call(
        functools.partial(
            gather_kernel, count, across, width, half, tile, raw_rows, parts, batches, pieces
        ),
        in_specs=[hbm] * 8,
        out_specs=[vmem] * 10,
        out_shape=[pltpu.VMEM((count * rows, w), jnp.bfloat16) for w in wides]
        + [pltpu.VMEM((rows, w), jnp.float32) for w in wides]
        + [pltpu.VMEM((1, w), jnp.float32) for w in wides]
        + [pltpu.VMEM((count * across, 1, piece), jnp.float32)],
        scratch_shapes=[pltpu.VMEM(a.shape, jnp.float32) for a in arrays]
        + [
            pltpu.VMEM((1, piece), jnp.float32),
            pltpu.VMEM((1, piece), jnp.float32),
            pltpu.VMEM((count, 1, sum(wides)), jnp.float32),
            pltpu.VMEM((2, raw_rows, width), jnp.float32),
            dma((len(batches), 2)),
            dma((2,)),
            dma((1,)),
            dma((len(parts),)),
            dma((2,)),
            dma((2,)),
            dma((2,)),
            dma((2,)),
            dma((2, 2)),
            dma((2, 3, len(pieces))),
        ],
        compiler_params=pltpu.CompilerParams(
            collective_id=0, has_side_effects=True,
            vmem_limit_bytes=4 * sum(a.size for a in arrays) + 2**21,
        ),
    )(*arrays, norm_train.reshape(1, piece), norm_step.reshape(1, piece))


def pieces_of(source, target, sem, cuts):
    size = source.shape[0] // cuts
    copies = []
    for c in range(cuts):
        at = pl.ds(c * size, size)
        copies.append(pltpu.make_async_copy(source.at[at], target.at[at], sem.at[c]))
    return copies


def early_key(count, rows):
    half = rows // 2
    return [pl.ds(i * half, cut_of(half)) for i in range(2 * count)]


def store_kernel(
    count, cuts,
    rk, rv, lq, lk, lv, scale_q, scale_k, scale_v, norm, rq,
    out_rk, out_rv, out_lq, out_lk, out_lv, out_sq, out_sk, out_sv, out_norm,
    sem, key_sem, own_sem,
):
    late = lax.rem(lax.axis_index("width"), 2) == 1
    rows = rv.shape[0] // count
    base = lax.axis_index("zero") * rows
    half = rows // 2
    cut = cut_of(half)
    both, last, first = [], [], []
    for i, (source, target) in enumerate(((lq, out_lq), (lk, out_lk), (lv, out_lv))):
        both += pieces_of(source, target, sem.at[i], cuts)
    first += pieces_of(rk, out_rk, sem.at[3], cuts) + pieces_of(rv, out_rv, sem.at[4], cuts)
    for i, at in enumerate(early_key(count, rows)):
        last.append(pltpu.make_async_copy(rk.at[at], out_rk.at[at], key_sem.at[i]))
    at = pl.ds(pl.multiple_of(base, 16), rows)
    last.append(pltpu.make_async_copy(rv.at[at], out_rv.at[at], own_sem.at[0]))
    for way in range(2):
        at = pl.ds(pl.multiple_of(base + way * half + cut, 16), half - cut)
        last.append(pltpu.make_async_copy(rk.at[at], out_rk.at[at], own_sem.at[1 + way]))

    for copy in both:
        copy.start()

    @pl.when(late)
    def _():
        for copy in last:
            copy.start()

    @pl.when(jnp.logical_not(late))
    def _():
        for copy in first:
            copy.start()

    for source, target in ((scale_q, out_sq), (scale_k, out_sk), (scale_v, out_sv)):
        target[...] = source[0, :]
    out_norm[...] = norm[...].astype(jnp.bfloat16)
    for copy in both:
        copy.wait()

    @pl.when(late)
    def _():
        for copy in last:
            copy.wait()

    @pl.when(jnp.logical_not(late))
    def _():
        for copy in first:
            copy.wait()


def store(arrays, count):
    cuts = 8
    dma = pltpu.SemaphoreType.DMA
    hbm = pl.BlockSpec(memory_space=pltpu.HBM)
    vmem = pl.BlockSpec(memory_space=pltpu.VMEM)
    return pl.pallas_call(
        functools.partial(store_kernel, count, cuts),
        in_specs=[vmem] * (len(arrays) - 1) + [hbm],
        out_specs=[hbm] * 5 + [vmem] * 4,
        out_shape=[jax.ShapeDtypeStruct(a.shape, a.dtype) for a in arrays[:5]]
        + [jax.ShapeDtypeStruct((a.shape[1],), a.dtype) for a in arrays[5:8]]
        + [jax.ShapeDtypeStruct(arrays[8].shape, jnp.bfloat16)],
        scratch_shapes=[dma((5, cuts)), dma((2 * count,)), dma((3,))],
        compiler_params=pltpu.CompilerParams(vmem_limit_bytes=2 * arrays[-1].size + 2**20),
    )(*arrays)


def store_one_kernel(cuts, source, target, sem):
    copies = pieces_of(source, target, sem, cuts)
    for copy in copies:
        copy.start()
    for copy in copies:
        copy.wait()


def store_one(array):
    cuts = 8
    return pl.pallas_call(
        functools.partial(store_one_kernel, cuts),
        in_specs=[pl.BlockSpec(memory_space=pltpu.VMEM)],
        out_specs=pl.BlockSpec(memory_space=pltpu.HBM),
        out_shape=jax.ShapeDtypeStruct(array.shape, array.dtype),
        scratch_shapes=[pltpu.SemaphoreType.DMA((cuts,))],
        compiler_params=pltpu.CompilerParams(vmem_limit_bytes=2**20),
    )(array)


def late_kernel(count, half, tile, own_k, own_v, after, rk, rv, load_sem, send_sem, recv_sem):
    me, node = ring_of(count)
    side = lax.axis_index("width")
    ahead, behind = node(1), node(-1)
    cut = cut_of(half)
    rest = half - cut
    pieces = [(rk, rest, t * tile) for t in range(rest // tile)]
    pieces += [(rv, half, t * tile) for t in range(half // tile)]

    def ring_copy(owner, step, p, way):
        ref, size, first = pieces[p]
        piece = ref.at[pl.ds(pl.multiple_of((owner * 2 + way) * size + first, 16), tile)]
        return pltpu.make_async_remote_copy(
            src_ref=piece, dst_ref=piece,
            send_sem=send_sem.at[way, lax.rem(step, 2)], recv_sem=recv_sem.at[way, lax.rem(step, 3), p],
            device_id=(behind if way else ahead, side), device_id_type=MESH,
        )

    def owner_of(step, way):
        return node(step if way else -step)

    def leave(step):
        whole = rv.at[pl.ds(0, rest + half)]
        for way in range(2):
            pltpu.make_async_remote_copy(
                src_ref=whole, dst_ref=whole, send_sem=send_sem.at[way, lax.rem(step, 2)],
                recv_sem=recv_sem.at[way, 0, 0], device_id=(ahead, side), device_id_type=MESH,
            ).wait_send()

    @pl.when(lax.rem(side, 2) == 1)
    def _():
        barrier = pltpu.get_barrier_semaphore()
        for other in (ahead, behind):
            pl.semaphore_signal(barrier, inc=1, device_id=(other, side), device_id_type=MESH)
        loads = []
        for way in range(2):
            there = pl.ds(pl.multiple_of((me * 2 + way) * half + cut, 16), rest)
            here = pl.ds(pl.multiple_of((me * 2 + way) * rest, 16), rest)
            loads.append(pltpu.make_async_copy(own_k.at[there], rk.at[here], load_sem.at[0, way]))
            at = pl.ds(pl.multiple_of((me * 2 + way) * half, 16), half)
            loads.append(pltpu.make_async_copy(own_v.at[at], rv.at[at], load_sem.at[1, way]))
        for load in loads:
            load.start()
        for load in loads:
            load.wait()
        pl.semaphore_wait(barrier, 2)
        for p in range(len(pieces)):
            for way in range(2):
                ring_copy(me, 0, p, way).start()

        def forward(step, carry):
            for p in range(len(pieces)):
                for way in range(2):
                    ring_copy(owner_of(step, way), step - 1, p, way).wait_recv()
                    ring_copy(owner_of(step, way), step, p, way).start()
            leave(step - 1)
            return carry

        lax.fori_loop(1, count - 1, forward, 0)
        for p in range(len(pieces)):
            for way in range(2):
                ring_copy(owner_of(count - 1, way), count - 2, p, way).wait_recv()
        leave(count - 2)


def gather_late(own_k, own_v, after, count):
    half = own_k.shape[0] // count // 2
    rest = half - cut_of(half)
    tile = 112 if rest % 112 == 0 and half % 112 == 0 else 16
    n = (rest + half) // tile
    hbm = pl.BlockSpec(memory_space=pltpu.HBM)
    vmem = pl.BlockSpec(memory_space=pltpu.VMEM)
    dma = pltpu.SemaphoreType.DMA
    return pl.pallas_call(
        functools.partial(late_kernel, count, half, tile),
        in_specs=[hbm] * 3,
        out_specs=[vmem] * 2,
        out_shape=[
            pltpu.VMEM((2 * count * rest, own_k.shape[1]), own_k.dtype),
            pltpu.VMEM(own_v.shape, own_v.dtype),
        ],
        scratch_shapes=[dma((2, 2)), dma((2, 2)), dma((2, 3, n))],
        compiler_params=pltpu.CompilerParams(
            collective_id=1, has_side_effects=True, vmem_limit_bytes=56 * 2**20
        ),
    )(own_k, own_v, after)


def store_late_kernel(count, rk, rv, start_k, start_v, out_k, out_v, sem):
    me, side = lax.axis_index("zero"), lax.axis_index("width")
    rows, rest = rv.shape[0] // count, rk.shape[0] // count // 2
    half = rows // 2

    @pl.when(lax.rem(side, 2) == 1)
    def _():
        for k in range(1, count):
            owner = lax.rem(me + k, count)
            at = pl.ds(pl.multiple_of(owner * rows, 16), rows)
            pltpu.make_async_copy(rv.at[at], out_v.at[at], sem.at[0]).start()
            for way in range(2):
                here = pl.ds(pl.multiple_of((owner * 2 + way) * rest, 16), rest)
                there = pl.ds(pl.multiple_of(owner * rows + way * half + half - rest, 16), rest)
                pltpu.make_async_copy(rk.at[here], out_k.at[there], sem.at[1]).start()
        for i, (near, far) in enumerate(((rv, out_v), (rk, out_k))):
            n = near.shape[0] // count * (count - 1)
            pltpu.make_async_copy(near.at[pl.ds(0, n)], far.at[pl.ds(0, n)], sem.at[i]).wait()


def store_late(rk, rv, start_k, start_v, count):
    hbm = pl.BlockSpec(memory_space=pltpu.HBM)
    vmem = pl.BlockSpec(memory_space=pltpu.VMEM)
    dma = pltpu.SemaphoreType.DMA
    return pl.pallas_call(
        functools.partial(store_late_kernel, count),
        in_specs=[vmem] * 2 + [hbm] * 2,
        out_specs=[hbm] * 2,
        out_shape=[jax.ShapeDtypeStruct(a.shape, a.dtype) for a in (start_k, start_v)],
        scratch_shapes=[dma((2,))],
        input_output_aliases={2: 0, 3: 1},
        compiler_params=pltpu.CompilerParams(vmem_limit_bytes=40 * 2**20),
    )(rk, rv, start_k, start_v)


def solution(mesh):
    count, across = mesh.shape["zero"], mesh.shape["width"]

    def body(
        train_query, slow_query, train_key, slow_key, train_value, slow_value, norm_train, norm_step
    ):
        arrays = gather(
            (train_query, slow_query, train_key, slow_key, train_value, slow_value),
            norm_train, norm_step, count, across,
        )
        rq = store_one(arrays[0])
        rk, rv, lq, lk, lv, *scales, norm = store((*arrays[1:], rq), count)
        serve_norm = norm.reshape(-1)
        rk, rv = store_late(*gather_late(rk, rv, serve_norm, count), rk, rv, count)
        return (rq, rk, rv, *scales, serve_norm, lq, lk, lv)

    in_specs = (P("zero", "width"),) * 6 + (P(("zero", "width")),) * 2
    out_specs = (
        (P(None, "width"),) * 3 + (P("width"),) * 3 + (P(),) + (P("zero", "width"),) * 3
    )
    return jax.shard_map(body, mesh=mesh, in_specs=in_specs, out_specs=out_specs, check_vma=False)
```

```python
import functools

import jax
import jax.numpy as jnp
from jax import lax
from jax.experimental import pallas as pl
from jax.experimental.pallas import tpu as pltpu
from jax.sharding import PartitionSpec as P

keep_rate = 0.5
MESH = pl.DeviceIdType.MESH


def grid_of(count):
    fast = 1
    while (2 * fast) ** 2 <= count and count % (2 * fast) == 0:
        fast *= 2
    return count // fast, fast


def node_at(place, slow, fast):
    if fast == 1:
        return place
    deep = slow - 1
    back = place // (deep * fast)
    column = place // deep
    step = place % deep
    step = step + (column % 2) * (deep - 1 - 2 * step)
    z = (1 - back) * (1 + step)
    y = (1 - back) * column + back * (fast - 1 - (place - deep * fast))
    return z * fast + y


def place_of(node, slow, fast):
    if fast == 1:
        return node
    deep = slow - 1
    z, y = node // fast, node % fast
    out = (z + slow - 1) // slow
    step = z - 1
    step = step + (y % 2) * (deep - 1 - 2 * step)
    return out * (y * deep + step) + (1 - out) * (deep * fast + fast - 1 - y)


def ring_of(count):
    me = lax.axis_index("zero")
    slow, fast = grid_of(count)
    place = place_of(me, slow, fast)

    def node(step):
        return node_at(lax.rem(place + count + step, count), slow, fast)

    return me, node


def gather_kernel(
    count, across, width, half, tile, raw_rows, parts, batches, pieces,
    tq, sq, tk, sk, tv, sv, norm_train, norm_step,
    rq, rk, rv, lq, lk, lv, scale_q, scale_k, scale_v, norm_all,
    itq, isq, itk, isk, itv, isv, in_train, in_step, stats, raw,
    load_sem, norm_sem, stat_send, stat_recv, near_sem, far_sem, raw_send, raw_recv,
    send_sem, recv_sem,
):
    me, node = ring_of(count)
    side = lax.axis_index("width")
    late = lax.rem(side, 2) == 1
    ahead, behind = node(1), node(-1)
    rows = 2 * half
    trains, slows = ((tq, itq), (tk, itk), (tv, itv)), ((sq, isq), (sk, isk), (sv, isv))
    latest, ready, scales = (lq, lk, lv), (rq, rk, rv), (scale_q, scale_k, scale_v)
    groups = [group for part in parts for group in part]

    def columns(c, n=1):
        return pl.ds(c * width, n * width)

    def allowed(p, action):
        if pieces[p][5]:
            pl.when(jnp.logical_not(late))(action)
        else:
            action()

    barrier = pltpu.get_barrier_semaphore()
    for k in range(1, count):
        pl.semaphore_signal(
            barrier, inc=1, device_id=(lax.rem(me + k, count), side), device_id_type=MESH
        )
    for k in range(1, across):
        pl.semaphore_signal(
            barrier, inc=1, device_id=(me, lax.rem(side + k, across)), device_id_type=MESH
        )

    loads = []
    for i, (_, which, c, n) in enumerate(batches):
        for j, arrays in enumerate((trains, slows)):
            far, near = arrays[which]
            loads.append(
                pltpu.make_async_copy(
                    far.at[:, columns(c, n)], near.at[:, columns(c, n)], load_sem.at[i, j]
                )
            )
            loads[-1].start()
    norms = [
        pltpu.make_async_copy(far, near, norm_sem.at[j])
        for j, (far, near) in enumerate(((norm_train, in_train), (norm_step, in_step)))
    ]
    for load in norms:
        load.start()
    mine = me * across + side

    def part_columns(part):
        first = groups.index(parts[part][0])
        return columns(first, len(parts[part]))

    def stat_copy(part, k):
        piece = stats.at[me, :, part_columns(part)]
        return pltpu.make_async_remote_copy(
            src_ref=piece, dst_ref=piece, send_sem=stat_send.at[0], recv_sem=stat_recv.at[part],
            device_id=(lax.rem(me + k, count), side), device_id_type=MESH,
        )

    def all_stats(part=None):
        piece = stats.at[pl.ds(0, count - 1)]
        if part is not None:
            piece = stats.at[pl.ds(0, count - 1), :, part_columns(part)]
        return pltpu.make_async_remote_copy(
            src_ref=piece, dst_ref=piece, send_sem=stat_send.at[0],
            recv_sem=stat_recv.at[part or 0], device_id=(ahead, side), device_id_type=MESH,
        )

    def near_copy(at, k=1):
        return pltpu.make_async_remote_copy(
            src_ref=norm_all.at[at], dst_ref=norm_all.at[at],
            send_sem=near_sem.at[0], recv_sem=near_sem.at[1],
            device_id=(me, lax.rem(side + k, across)), device_id_type=MESH,
        )

    def far_copy(at, k=1):
        return pltpu.make_async_remote_copy(
            src_ref=norm_all.at[at], dst_ref=norm_all.at[at],
            send_sem=far_sem.at[0], recv_sem=far_sem.at[1],
            device_id=(lax.rem(me + k, count), side), device_id_type=MESH,
        )

    all_near = near_copy(pl.ds(0, across - 1))
    all_far = far_copy(pl.ds(0, (count - 1) * across))

    def average(i):
        which, c = groups[i]

        def step(t, total):
            at = pl.ds(pl.multiple_of(t * tile, 16), tile)
            value = (
                keep_rate * slows[which][1][at, columns(c)]
                + (1.0 - keep_rate) * trains[which][1][at, columns(c)]
            )
            latest[which][at, columns(c)] = value
            return total + jnp.sum((value * value).reshape(tile // 8, 8, width), axis=0)

        total = lax.fori_loop(0, rows // tile, step, jnp.zeros((8, width), jnp.float32))
        stats[me, :, columns(i)] = jnp.sum(total, axis=0, keepdims=True)

    def averages(part):
        for i, batch in enumerate(batches):
            if batch[0] == part:
                loads[2 * i].wait()
                loads[2 * i + 1].wait()
        for group in parts[part]:
            average(groups.index(group))

    def ring_copy(owner, step, p, way):
        which, c, n, first, size, _ = pieces[p]
        spot = pl.ds(pl.multiple_of(owner * rows + way * half + first, 16), size)
        piece = ready[which].at[spot, columns(c, n)]
        return pltpu.make_async_remote_copy(
            src_ref=piece, dst_ref=piece,
            send_sem=send_sem.at[way, lax.rem(step, 2)],
            recv_sem=recv_sem.at[way, lax.rem(step, 3), p],
            device_id=(behind if way else ahead, side), device_id_type=MESH,
        )

    def raw_copy(way):
        return pltpu.make_async_remote_copy(
            src_ref=lk.at[pl.ds(way * half, raw_rows)], dst_ref=raw.at[way],
            send_sem=raw_send.at[way], recv_sem=raw_recv.at[way],
            device_id=(behind if way else ahead, side), device_id_type=MESH,
        )

    def owner_of(step, way):
        return node(step if way else -step)

    def send_own(part):
        for p in (*range(1, len(pieces)), 0):
            which, c, n, first, size, _ = pieces[p]
            if (which, c) not in parts[part]:
                continue
            for way in range(2):
                for each in range(c, c + n):
                    scale = scales[which][:, columns(each)]
                    short = tile if size % tile == 0 else 16

                    def step(t, carry):
                        at = pl.multiple_of(way * half + first + t * short, 16)
                        home = pl.multiple_of(me * rows + at, 16)
                        ready[which][pl.ds(home, short), columns(each)] = (
                            latest[which][pl.ds(at, short), columns(each)] / scale
                        ).astype(jnp.bfloat16)
                        return carry

                    lax.fori_loop(0, size // short, step, 0)
                if p:
                    allowed(p, lambda: ring_copy(me, 0, p, way).start())

    def tell(part):
        for k in range(1, count):
            stat_copy(part, k).start()

    def finish(part):
        all_stats(part).wait_recv()
        for group in parts[part]:
            i = groups.index(group)
            which, c = group
            total = stats[0, :, columns(i)]
            for k in range(1, count):
                total = total + stats[k, :, columns(i)]
            scales[which][:, columns(c)] = jnp.sqrt(total)

    for part in range(len(parts)):
        averages(part)
        if part == 0:
            pl.semaphore_wait(barrier, count + across - 2)
        tell(part)
        if part == 0:
            for way in range(2):
                raw_copy(way).start()
            for load in norms:
                load.wait()
            norm_all[mine] = in_train[...] + in_step[...]
            for k in range(1, across):
                near_copy(mine, k).start()
        else:
            finish(part - 1)
            send_own(part - 1)
    finish(len(parts) - 1)
    send_own(len(parts) - 1)
    all_near.wait_recv()
    for k in range(1, count):
        far_copy(pl.ds(me * across, across), k).start()

    def leave(step):
        def left(n):
            whole = rk.at[pl.ds(0, n)]
            for way in range(2):
                pltpu.make_async_remote_copy(
                    src_ref=whole, dst_ref=whole, send_sem=send_sem.at[way, lax.rem(step, 2)],
                    recv_sem=recv_sem.at[way, 0, 0], device_id=(ahead, side), device_id_type=MESH,
                ).wait_send()

        for kind in (late, jnp.logical_not(late)):
            n = sum(p[2] * p[4] for p in pieces if kind is not late or not p[5])
            pl.when(jnp.logical_and(kind, step > 0))(functools.partial(left, n))
            pl.when(jnp.logical_and(kind, step == 0))(functools.partial(left, n - raw_rows))

    def pass_raw():
        short = tile if raw_rows % tile == 0 else 16
        for way in range(2):
            raw_copy(way).wait_recv()
            home = owner_of(1, way) * rows + way * half

            def step(t, carry):
                at = pl.ds(pl.multiple_of(t * short, 16), short)
                rk[pl.ds(pl.multiple_of(home + t * short, 16), short), :] = (
                    raw[way, at, :] / scale_k[...]
                ).astype(jnp.bfloat16)
                return carry

            lax.fori_loop(0, raw_rows // short, step, 0)
            ring_copy(owner_of(1, way), 1, 0, way).start()

    def forward(step, carry):
        owners = owner_of(step, 0), owner_of(step, 1)
        for p in range(len(pieces)):

            def pass_on():
                for way in range(2):
                    ring_copy(owners[way], step - 1, p, way).wait_recv()
                    ring_copy(owners[way], step, p, way).start()

            if p:
                allowed(p, pass_on)
            else:
                pl.when(step > 1)(pass_on)
        leave(step - 1)
        return carry

    pass_raw()
    lax.fori_loop(1, count - 1, forward, 0)
    for way in range(2):
        raw_copy(way).wait_send()
    all_stats().wait_send()
    all_near.wait_send()
    all_far.wait_send()
    all_far.wait_recv()
    for p in range(len(pieces)):

        def arrive():
            for way in range(2):
                ring_copy(owner_of(count - 1, way), count - 2, p, way).wait_recv()

        allowed(p, arrive)
    leave(count - 2)


def cut_of(half):
    return half - (112 if half % 112 == 0 and half > 112 else half // 64 * 16)


def gather(arrays, norm_train, norm_step, count, across):
    rows = arrays[0].shape[0]
    wides = [a.shape[1] for a in arrays[::2]]
    half = rows // 2
    cut = cut_of(half)
    raw_rows = cut // 32 * 16
    width = wides[1]
    tile = 112 if half % 112 == 0 else 16
    n = wides[0] // width
    a, b = 1, (n + 1) // 2
    spans = [(0, 0, a), (0, a, b - a), (0, b, n - b)]
    parts = [[(which, c + i) for i in range(m)] for which, c, m in spans]
    parts[0].append((1, 0))
    parts[2].append((2, 0))
    batches = [(0, 1, 0, 1)] + [(i, *span) for i, span in enumerate(spans)] + [(2, 2, 0, 1)]
    pieces = [(1, 0, 1, 0, raw_rows, False), (*spans[0], 0, half, False)]
    pieces += [(1, 0, 1, raw_rows, cut - raw_rows, False), (1, 0, 1, cut, half - cut, True)]
    pieces += [(*span, 0, half, False) for span in spans[1:]] + [(2, 0, 1, 0, half, True)]
    piece = norm_train.shape[0]
    hbm = pl.BlockSpec(memory_space=pl.ANY)
    vmem = pl.BlockSpec(memory_space=pltpu.VMEM)
    dma = pltpu.SemaphoreType.DMA
    return pl.pallas_call(
        functools.partial(
            gather_kernel, count, across, width, half, tile, raw_rows, parts, batches, pieces
        ),
        in_specs=[hbm] * 8,
        out_specs=[vmem] * 10,
        out_shape=[pltpu.VMEM((count * rows, w), jnp.bfloat16) for w in wides]
        + [pltpu.VMEM((rows, w), jnp.float32) for w in wides]
        + [pltpu.VMEM((1, w), jnp.float32) for w in wides]
        + [pltpu.VMEM((count * across, 1, piece), jnp.float32)],
        scratch_shapes=[pltpu.VMEM(a.shape, jnp.float32) for a in arrays]
        + [
            pltpu.VMEM((1, piece), jnp.float32),
            pltpu.VMEM((1, piece), jnp.float32),
            pltpu.VMEM((count, 1, sum(wides)), jnp.float32),
            pltpu.VMEM((2, raw_rows, width), jnp.float32),
            dma((len(batches), 2)),
            dma((2,)),
            dma((1,)),
            dma((len(parts),)),
            dma((2,)),
            dma((2,)),
            dma((2,)),
            dma((2,)),
            dma((2, 2)),
            dma((2, 3, len(pieces))),
        ],
        compiler_params=pltpu.CompilerParams(
            collective_id=0, has_side_effects=True,
            vmem_limit_bytes=4 * sum(a.size for a in arrays) + 2**21,
        ),
    )(*arrays, norm_train.reshape(1, piece), norm_step.reshape(1, piece))


def pieces_of(source, target, sem, cuts):
    size = source.shape[0] // cuts
    copies = []
    for c in range(cuts):
        at = pl.ds(c * size, size)
        copies.append(pltpu.make_async_copy(source.at[at], target.at[at], sem.at[c]))
    return copies


def early_key(count, rows):
    half = rows // 2
    return [pl.ds(i * half, cut_of(half)) for i in range(2 * count)]


def store_kernel(
    count, cuts,
    rk, rv, lq, lk, lv, scale_q, scale_k, scale_v, norm, rq,
    out_rk, out_rv, out_lq, out_lk, out_lv, out_sq, out_sk, out_sv, out_norm,
    sem, key_sem, own_sem,
):
    late = lax.rem(lax.axis_index("width"), 2) == 1
    rows = rv.shape[0] // count
    base = lax.axis_index("zero") * rows
    half = rows // 2
    cut = cut_of(half)
    both, last, first = [], [], []
    for i, (source, target) in enumerate(((lq, out_lq), (lk, out_lk), (lv, out_lv))):
        both += pieces_of(source, target, sem.at[i], cuts)
    first += pieces_of(rk, out_rk, sem.at[3], cuts) + pieces_of(rv, out_rv, sem.at[4], cuts)
    for i, at in enumerate(early_key(count, rows)):
        last.append(pltpu.make_async_copy(rk.at[at], out_rk.at[at], key_sem.at[i]))
    at = pl.ds(pl.multiple_of(base, 16), rows)
    last.append(pltpu.make_async_copy(rv.at[at], out_rv.at[at], own_sem.at[0]))
    for way in range(2):
        at = pl.ds(pl.multiple_of(base + way * half + cut, 16), half - cut)
        last.append(pltpu.make_async_copy(rk.at[at], out_rk.at[at], own_sem.at[1 + way]))

    for copy in both:
        copy.start()

    @pl.when(late)
    def _():
        for copy in last:
            copy.start()

    @pl.when(jnp.logical_not(late))
    def _():
        for copy in first:
            copy.start()

    for source, target in ((scale_q, out_sq), (scale_k, out_sk), (scale_v, out_sv)):
        target[...] = source[0, :]
    out_norm[...] = norm[...].astype(jnp.bfloat16)
    for copy in both:
        copy.wait()

    @pl.when(late)
    def _():
        for copy in last:
            copy.wait()

    @pl.when(jnp.logical_not(late))
    def _():
        for copy in first:
            copy.wait()


def store(arrays, count):
    cuts = 8
    dma = pltpu.SemaphoreType.DMA
    hbm = pl.BlockSpec(memory_space=pltpu.HBM)
    vmem = pl.BlockSpec(memory_space=pltpu.VMEM)
    return pl.pallas_call(
        functools.partial(store_kernel, count, cuts),
        in_specs=[vmem] * (len(arrays) - 1) + [hbm],
        out_specs=[hbm] * 5 + [vmem] * 4,
        out_shape=[jax.ShapeDtypeStruct(a.shape, a.dtype) for a in arrays[:5]]
        + [jax.ShapeDtypeStruct((a.shape[1],), a.dtype) for a in arrays[5:8]]
        + [jax.ShapeDtypeStruct(arrays[8].shape, jnp.bfloat16)],
        scratch_shapes=[dma((5, cuts)), dma((2 * count,)), dma((3,))],
        compiler_params=pltpu.CompilerParams(vmem_limit_bytes=2 * arrays[-1].size + 2**20),
    )(*arrays)


def store_one_kernel(cuts, source, target, sem):
    copies = pieces_of(source, target, sem, cuts)
    for copy in copies:
        copy.start()
    for copy in copies:
        copy.wait()


def store_one(array):
    cuts = 8
    return pl.pallas_call(
        functools.partial(store_one_kernel, cuts),
        in_specs=[pl.BlockSpec(memory_space=pltpu.VMEM)],
        out_specs=pl.BlockSpec(memory_space=pltpu.HBM),
        out_shape=jax.ShapeDtypeStruct(array.shape, array.dtype),
        scratch_shapes=[pltpu.SemaphoreType.DMA((cuts,))],
        compiler_params=pltpu.CompilerParams(vmem_limit_bytes=2**20),
    )(array)


def late_kernel(count, half, tile, own_k, own_v, after, rk, rv, load_sem, send_sem, recv_sem):
    me, node = ring_of(count)
    side = lax.axis_index("width")
    ahead, behind = node(1), node(-1)
    cut = cut_of(half)
    rest = half - cut
    pieces = [(rk, rest, t * tile) for t in range(rest // tile)]
    pieces += [(rv, half, t * tile) for t in range(half // tile)]

    def ring_copy(owner, step, p, way):
        ref, size, first = pieces[p]
        piece = ref.at[pl.ds(pl.multiple_of((owner * 2 + way) * size + first, 16), tile)]
        return pltpu.make_async_remote_copy(
            src_ref=piece, dst_ref=piece,
            send_sem=send_sem.at[way, lax.rem(step, 2)], recv_sem=recv_sem.at[way, lax.rem(step, 3), p],
            device_id=(behind if way else ahead, side), device_id_type=MESH,
        )

    def owner_of(step, way):
        return node(step if way else -step)

    def leave(step):
        whole = rv.at[pl.ds(0, rest + half)]
        for way in range(2):
            pltpu.make_async_remote_copy(
                src_ref=whole, dst_ref=whole, send_sem=send_sem.at[way, lax.rem(step, 2)],
                recv_sem=recv_sem.at[way, 0, 0], device_id=(ahead, side), device_id_type=MESH,
            ).wait_send()

    @pl.when(lax.rem(side, 2) == 1)
    def _():
        barrier = pltpu.get_barrier_semaphore()
        for other in (ahead, behind):
            pl.semaphore_signal(barrier, inc=1, device_id=(other, side), device_id_type=MESH)
        loads = []
        for way in range(2):
            there = pl.ds(pl.multiple_of((me * 2 + way) * half + cut, 16), rest)
            here = pl.ds(pl.multiple_of((me * 2 + way) * rest, 16), rest)
            loads.append(pltpu.make_async_copy(own_k.at[there], rk.at[here], load_sem.at[0, way]))
            at = pl.ds(pl.multiple_of((me * 2 + way) * half, 16), half)
            loads.append(pltpu.make_async_copy(own_v.at[at], rv.at[at], load_sem.at[1, way]))
        for load in loads:
            load.start()
        for load in loads:
            load.wait()
        pl.semaphore_wait(barrier, 2)
        for p in range(len(pieces)):
            for way in range(2):
                ring_copy(me, 0, p, way).start()

        def forward(step, carry):
            for p in range(len(pieces)):
                for way in range(2):
                    ring_copy(owner_of(step, way), step - 1, p, way).wait_recv()
                    ring_copy(owner_of(step, way), step, p, way).start()
            leave(step - 1)
            return carry

        lax.fori_loop(1, count - 1, forward, 0)
        for p in range(len(pieces)):
            for way in range(2):
                ring_copy(owner_of(count - 1, way), count - 2, p, way).wait_recv()
        leave(count - 2)


def gather_late(own_k, own_v, after, count):
    half = own_k.shape[0] // count // 2
    rest = half - cut_of(half)
    tile = 112 if rest % 112 == 0 and half % 112 == 0 else 16
    n = (rest + half) // tile
    hbm = pl.BlockSpec(memory_space=pltpu.HBM)
    vmem = pl.BlockSpec(memory_space=pltpu.VMEM)
    dma = pltpu.SemaphoreType.DMA
    return pl.pallas_call(
        functools.partial(late_kernel, count, half, tile),
        in_specs=[hbm] * 3,
        out_specs=[vmem] * 2,
        out_shape=[
            pltpu.VMEM((2 * count * rest, own_k.shape[1]), own_k.dtype),
            pltpu.VMEM(own_v.shape, own_v.dtype),
        ],
        scratch_shapes=[dma((2, 2)), dma((2, 2)), dma((2, 3, n))],
        compiler_params=pltpu.CompilerParams(
            collective_id=1, has_side_effects=True, vmem_limit_bytes=56 * 2**20
        ),
    )(own_k, own_v, after)


def store_late_kernel(count, rk, rv, start_k, start_v, out_k, out_v, sem):
    me, side = lax.axis_index("zero"), lax.axis_index("width")
    rows, rest = rv.shape[0] // count, rk.shape[0] // count // 2
    half = rows // 2

    @pl.when(lax.rem(side, 2) == 1)
    def _():
        for k in range(1, count):
            owner = lax.rem(me + k, count)
            at = pl.ds(pl.multiple_of(owner * rows, 16), rows)
            pltpu.make_async_copy(rv.at[at], out_v.at[at], sem.at[0]).start()
            for way in range(2):
                here = pl.ds(pl.multiple_of((owner * 2 + way) * rest, 16), rest)
                there = pl.ds(pl.multiple_of(owner * rows + way * half + half - rest, 16), rest)
                pltpu.make_async_copy(rk.at[here], out_k.at[there], sem.at[1]).start()
        for i, (near, far) in enumerate(((rv, out_v), (rk, out_k))):
            n = near.shape[0] // count * (count - 1)
            pltpu.make_async_copy(near.at[pl.ds(0, n)], far.at[pl.ds(0, n)], sem.at[i]).wait()


def store_late(rk, rv, start_k, start_v, count):
    hbm = pl.BlockSpec(memory_space=pltpu.HBM)
    vmem = pl.BlockSpec(memory_space=pltpu.VMEM)
    dma = pltpu.SemaphoreType.DMA
    return pl.pallas_call(
        functools.partial(store_late_kernel, count),
        in_specs=[vmem] * 2 + [hbm] * 2,
        out_specs=[hbm] * 2,
        out_shape=[jax.ShapeDtypeStruct(a.shape, a.dtype) for a in (start_k, start_v)],
        scratch_shapes=[dma((2,))],
        input_output_aliases={2: 0, 3: 1},
        compiler_params=pltpu.CompilerParams(vmem_limit_bytes=40 * 2**20),
    )(rk, rv, start_k, start_v)


def solution(mesh):
    count, across = mesh.shape["zero"], mesh.shape["width"]

    def body(
        train_query, slow_query, train_key, slow_key, train_value, slow_value, norm_train, norm_step
    ):
        arrays = gather(
            (train_query, slow_query, train_key, slow_key, train_value, slow_value),
            norm_train, norm_step, count, across,
        )
        rq = store_one(arrays[0])
        rk, rv, lq, lk, lv, *scales, norm = store((*arrays[1:], rq), count)
        serve_norm = norm.reshape(-1)
        rk, rv = store_late(*gather_late(rk, rv, serve_norm, count), rk, rv, count)
        return (rq, rk, rv, *scales, serve_norm, lq, lk, lv)

    in_specs = (P("zero", "width"),) * 6 + (P(("zero", "width")),) * 2
    out_specs = (
        (P(None, "width"),) * 3 + (P("width"),) * 3 + (P(),) + (P("zero", "width"),) * 3
    )
    return jax.shard_map(body, mesh=mesh, in_specs=in_specs, out_specs=out_specs, check_vma=False)
```

```python
import functools

import jax
import jax.numpy as jnp
from jax import lax
from jax.experimental import pallas as pl
from jax.experimental.pallas import tpu as pltpu
from jax.sharding import PartitionSpec as P

keep_rate = 0.5
MESH = pl.DeviceIdType.MESH


def grid_of(count):
    fast = 1
    while (2 * fast) ** 2 <= count and count % (2 * fast) == 0:
        fast *= 2
    return count // fast, fast


def node_at(place, slow, fast):
    if fast == 1:
        return place
    deep = slow - 1
    back = place // (deep * fast)
    column = place // deep
    step = place % deep
    step = step + (column % 2) * (deep - 1 - 2 * step)
    z = (1 - back) * (1 + step)
    y = (1 - back) * column + back * (fast - 1 - (place - deep * fast))
    return z * fast + y


def place_of(node, slow, fast):
    if fast == 1:
        return node
    deep = slow - 1
    z, y = node // fast, node % fast
    out = (z + slow - 1) // slow
    step = z - 1
    step = step + (y % 2) * (deep - 1 - 2 * step)
    return out * (y * deep + step) + (1 - out) * (deep * fast + fast - 1 - y)


def ring_of(count):
    me = lax.axis_index("zero")
    slow, fast = grid_of(count)
    place = place_of(me, slow, fast)

    def node(step):
        return node_at(lax.rem(place + count + step, count), slow, fast)

    return me, node


def gather_kernel(
    count, across, width, half, tile, raw_rows, parts, batches, pieces,
    tq, sq, tk, sk, tv, sv, norm_train, norm_step,
    rq, rk, rv, lq, lk, lv, scale_q, scale_k, scale_v, norm_all,
    itq, isq, itk, isk, itv, isv, in_train, in_step, stats, raw,
    load_sem, norm_sem, stat_send, stat_recv, near_sem, far_sem, raw_send, raw_recv,
    send_sem, recv_sem,
):
    me, node = ring_of(count)
    side = lax.axis_index("width")
    late = lax.rem(side, 2) == 1
    ahead, behind = node(1), node(-1)
    rows = 2 * half
    trains, slows = ((tq, itq), (tk, itk), (tv, itv)), ((sq, isq), (sk, isk), (sv, isv))
    latest, ready, scales = (lq, lk, lv), (rq, rk, rv), (scale_q, scale_k, scale_v)
    groups = [group for part in parts for group in part]

    def columns(c, n=1):
        return pl.ds(c * width, n * width)

    def allowed(p, action):
        if pieces[p][5]:
            pl.when(jnp.logical_not(late))(action)
        else:
            action()

    barrier = pltpu.get_barrier_semaphore()
    for k in range(1, count):
        pl.semaphore_signal(
            barrier, inc=1, device_id=(lax.rem(me + k, count), side), device_id_type=MESH
        )
    for k in range(1, across):
        pl.semaphore_signal(
            barrier, inc=1, device_id=(me, lax.rem(side + k, across)), device_id_type=MESH
        )

    loads = []
    for i, (_, which, c, n) in enumerate(batches):
        for j, arrays in enumerate((trains, slows)):
            far, near = arrays[which]
            loads.append(
                pltpu.make_async_copy(
                    far.at[:, columns(c, n)], near.at[:, columns(c, n)], load_sem.at[i, j]
                )
            )
            loads[-1].start()
    norms = [
        pltpu.make_async_copy(far, near, norm_sem.at[j])
        for j, (far, near) in enumerate(((norm_train, in_train), (norm_step, in_step)))
    ]
    for load in norms:
        load.start()
    mine = me * across + side

    def part_columns(part):
        first = groups.index(parts[part][0])
        return columns(first, len(parts[part]))

    def stat_copy(part, k):
        piece = stats.at[me, :, part_columns(part)]
        return pltpu.make_async_remote_copy(
            src_ref=piece, dst_ref=piece, send_sem=stat_send.at[0], recv_sem=stat_recv.at[part],
            device_id=(lax.rem(me + k, count), side), device_id_type=MESH,
        )

    def all_stats(part=None):
        piece = stats.at[pl.ds(0, count - 1)]
        if part is not None:
            piece = stats.at[pl.ds(0, count - 1), :, part_columns(part)]
        return pltpu.make_async_remote_copy(
            src_ref=piece, dst_ref=piece, send_sem=stat_send.at[0],
            recv_sem=stat_recv.at[part or 0], device_id=(ahead, side), device_id_type=MESH,
        )

    def near_copy(at, k=1):
        return pltpu.make_async_remote_copy(
            src_ref=norm_all.at[at], dst_ref=norm_all.at[at],
            send_sem=near_sem.at[0], recv_sem=near_sem.at[1],
            device_id=(me, lax.rem(side + k, across)), device_id_type=MESH,
        )

    def far_copy(at, k=1):
        return pltpu.make_async_remote_copy(
            src_ref=norm_all.at[at], dst_ref=norm_all.at[at],
            send_sem=far_sem.at[0], recv_sem=far_sem.at[1],
            device_id=(lax.rem(me + k, count), side), device_id_type=MESH,
        )

    all_near = near_copy(pl.ds(0, across - 1))
    all_far = far_copy(pl.ds(0, (count - 1) * across))

    def average(i):
        which, c = groups[i]

        def step(t, total):
            at = pl.ds(pl.multiple_of(t * tile, 16), tile)
            value = (
                keep_rate * slows[which][1][at, columns(c)]
                + (1.0 - keep_rate) * trains[which][1][at, columns(c)]
            )
            latest[which][at, columns(c)] = value
            return total + jnp.sum((value * value).reshape(tile // 8, 8, width), axis=0)

        total = lax.fori_loop(0, rows // tile, step, jnp.zeros((8, width), jnp.float32))
        stats[me, :, columns(i)] = jnp.sum(total, axis=0, keepdims=True)

    def averages(part):
        for i, batch in enumerate(batches):
            if batch[0] == part:
                loads[2 * i].wait()
                loads[2 * i + 1].wait()
        for group in parts[part]:
            average(groups.index(group))

    def ring_copy(owner, step, p, way):
        which, c, n, first, size, _ = pieces[p]
        spot = pl.ds(pl.multiple_of(owner * rows + way * half + first, 16), size)
        piece = ready[which].at[spot, columns(c, n)]
        return pltpu.make_async_remote_copy(
            src_ref=piece, dst_ref=piece,
            send_sem=send_sem.at[way, lax.rem(step, 2)],
            recv_sem=recv_sem.at[way, lax.rem(step, 3), p],
            device_id=(behind if way else ahead, side), device_id_type=MESH,
        )

    def raw_copy(way):
        return pltpu.make_async_remote_copy(
            src_ref=lk.at[pl.ds(way * half, raw_rows)], dst_ref=raw.at[way],
            send_sem=raw_send.at[way], recv_sem=raw_recv.at[way],
            device_id=(behind if way else ahead, side), device_id_type=MESH,
        )

    def owner_of(step, way):
        return node(step if way else -step)

    def send_own(part):
        for p in (*range(1, len(pieces)), 0):
            which, c, n, first, size, _ = pieces[p]
            if (which, c) not in parts[part]:
                continue
            for way in range(2):
                for each in range(c, c + n):
                    scale = scales[which][:, columns(each)]
                    short = tile if size % tile == 0 else 16

                    def step(t, carry):
                        at = pl.multiple_of(way * half + first + t * short, 16)
                        home = pl.multiple_of(me * rows + at, 16)
                        ready[which][pl.ds(home, short), columns(each)] = (
                            latest[which][pl.ds(at, short), columns(each)] / scale
                        ).astype(jnp.bfloat16)
                        return carry

                    lax.fori_loop(0, size // short, step, 0)
                if p:
                    allowed(p, lambda: ring_copy(me, 0, p, way).start())

    def tell(part):
        for k in range(1, count):
            stat_copy(part, k).start()

    def finish(part):
        all_stats(part).wait_recv()
        for group in parts[part]:
            i = groups.index(group)
            which, c = group
            total = stats[0, :, columns(i)]
            for k in range(1, count):
                total = total + stats[k, :, columns(i)]
            scales[which][:, columns(c)] = jnp.sqrt(total)

    for part in range(len(parts)):
        averages(part)
        if part == 0:
            pl.semaphore_wait(barrier, count + across - 2)
        tell(part)
        if part == 0:
            for way in range(2):
                raw_copy(way).start()
            for load in norms:
                load.wait()
            norm_all[mine] = in_train[...] + in_step[...]
            for k in range(1, across):
                near_copy(mine, k).start()
        else:
            finish(part - 1)
            send_own(part - 1)
    finish(len(parts) - 1)
    send_own(len(parts) - 1)
    all_near.wait_recv()
    for k in range(1, count):
        far_copy(pl.ds(me * across, across), k).start()

    def leave(step):
        def left(n):
            whole = rk.at[pl.ds(0, n)]
            for way in range(2):
                pltpu.make_async_remote_copy(
                    src_ref=whole, dst_ref=whole, send_sem=send_sem.at[way, lax.rem(step, 2)],
                    recv_sem=recv_sem.at[way, 0, 0], device_id=(ahead, side), device_id_type=MESH,
                ).wait_send()

        for kind in (late, jnp.logical_not(late)):
            n = sum(p[2] * p[4] for p in pieces if kind is not late or not p[5])
            pl.when(jnp.logical_and(kind, step > 0))(functools.partial(left, n))
            pl.when(jnp.logical_and(kind, step == 0))(functools.partial(left, n - raw_rows))

    def pass_raw():
        short = tile if raw_rows % tile == 0 else 16
        for way in range(2):
            raw_copy(way).wait_recv()
            home = owner_of(1, way) * rows + way * half

            def step(t, carry):
                at = pl.ds(pl.multiple_of(t * short, 16), short)
                rk[pl.ds(pl.multiple_of(home + t * short, 16), short), :] = (
                    raw[way, at, :] / scale_k[...]
                ).astype(jnp.bfloat16)
                return carry

            lax.fori_loop(0, raw_rows // short, step, 0)
            ring_copy(owner_of(1, way), 1, 0, way).start()

    def forward(step, carry):
        owners = owner_of(step, 0), owner_of(step, 1)
        for p in range(len(pieces)):

            def pass_on():
                for way in range(2):
                    ring_copy(owners[way], step - 1, p, way).wait_recv()
                    ring_copy(owners[way], step, p, way).start()

            if p:
                allowed(p, pass_on)
            else:
                pl.when(step > 1)(pass_on)
        leave(step - 1)
        return carry

    pass_raw()
    lax.fori_loop(1, count - 1, forward, 0)
    for way in range(2):
        raw_copy(way).wait_send()
    all_stats().wait_send()
    all_near.wait_send()
    all_far.wait_send()
    all_far.wait_recv()
    for p in range(len(pieces)):

        def arrive():
            for way in range(2):
                ring_copy(owner_of(count - 1, way), count - 2, p, way).wait_recv()

        allowed(p, arrive)
    leave(count - 2)


def cut_of(half):
    return half // 7 * 6 if half % 112 == 0 else half - half // 64 * 16


def gather(arrays, norm_train, norm_step, count, across):
    rows = arrays[0].shape[0]
    wides = [a.shape[1] for a in arrays[::2]]
    half = rows // 2
    cut = cut_of(half)
    raw_rows = min(160, cut // 32 * 16)
    width = wides[1]
    tile = 112 if half % 112 == 0 else 16
    n = wides[0] // width
    a, b = 1, (n + 1) // 2
    spans = [(0, 0, a), (0, a, b - a), (0, b, n - b)]
    parts = [[(which, c + i) for i in range(m)] for which, c, m in spans]
    parts[0].append((1, 0))
    parts[2].append((2, 0))
    batches = [(0, 1, 0, 1)] + [(i, *span) for i, span in enumerate(spans)] + [(2, 2, 0, 1)]
    pieces = [(1, 0, 1, 0, raw_rows, False), (*spans[0], 0, half, False)]
    pieces += [(1, 0, 1, raw_rows, cut - raw_rows, False), (1, 0, 1, cut, half - cut, True)]
    pieces += [(*span, 0, half, False) for span in spans[1:]] + [(2, 0, 1, 0, half, True)]
    piece = norm_train.shape[0]
    hbm = pl.BlockSpec(memory_space=pl.ANY)
    vmem = pl.BlockSpec(memory_space=pltpu.VMEM)
    dma = pltpu.SemaphoreType.DMA
    return pl.pallas_call(
        functools.partial(
            gather_kernel, count, across, width, half, tile, raw_rows, parts, batches, pieces
        ),
        in_specs=[hbm] * 8,
        out_specs=[vmem] * 10,
        out_shape=[pltpu.VMEM((count * rows, w), jnp.bfloat16) for w in wides]
        + [pltpu.VMEM((rows, w), jnp.float32) for w in wides]
        + [pltpu.VMEM((1, w), jnp.float32) for w in wides]
        + [pltpu.VMEM((count * across, 1, piece), jnp.float32)],
        scratch_shapes=[pltpu.VMEM(a.shape, jnp.float32) for a in arrays]
        + [
            pltpu.VMEM((1, piece), jnp.float32),
            pltpu.VMEM((1, piece), jnp.float32),
            pltpu.VMEM((count, 1, sum(wides)), jnp.float32),
            pltpu.VMEM((2, raw_rows, width), jnp.float32),
            dma((len(batches), 2)),
            dma((2,)),
            dma((1,)),
            dma((len(parts),)),
            dma((2,)),
            dma((2,)),
            dma((2,)),
            dma((2,)),
            dma((2, 2)),
            dma((2, 3, len(pieces))),
        ],
        compiler_params=pltpu.CompilerParams(
            collective_id=0, has_side_effects=True,
            vmem_limit_bytes=4 * sum(a.size for a in arrays) + 2**21,
        ),
    )(*arrays, norm_train.reshape(1, piece), norm_step.reshape(1, piece))


def pieces_of(source, target, sem, cuts):
    size = source.shape[0] // cuts
    copies = []
    for c in range(cuts):
        at = pl.ds(c * size, size)
        copies.append(pltpu.make_async_copy(source.at[at], target.at[at], sem.at[c]))
    return copies


def early_key(count, rows):
    half = rows // 2
    return [pl.ds(i * half, cut_of(half)) for i in range(2 * count)]


def store_kernel(
    count, cuts,
    rk, rv, lq, lk, lv, scale_q, scale_k, scale_v, norm, rq,
    out_rk, out_rv, out_lq, out_lk, out_lv, out_sq, out_sk, out_sv, out_norm,
    sem, key_sem, own_sem,
):
    late = lax.rem(lax.axis_index("width"), 2) == 1
    rows = rv.shape[0] // count
    base = lax.axis_index("zero") * rows
    half = rows // 2
    cut = cut_of(half)
    both, last, first = [], [], []
    for i, (source, target) in enumerate(((lq, out_lq), (lk, out_lk), (lv, out_lv))):
        both += pieces_of(source, target, sem.at[i], cuts)
    first += pieces_of(rk, out_rk, sem.at[3], cuts) + pieces_of(rv, out_rv, sem.at[4], cuts)
    for i, at in enumerate(early_key(count, rows)):
        last.append(pltpu.make_async_copy(rk.at[at], out_rk.at[at], key_sem.at[i]))
    at = pl.ds(pl.multiple_of(base, 16), rows)
    last.append(pltpu.make_async_copy(rv.at[at], out_rv.at[at], own_sem.at[0]))
    for way in range(2):
        at = pl.ds(pl.multiple_of(base + way * half + cut, 16), half - cut)
        last.append(pltpu.make_async_copy(rk.at[at], out_rk.at[at], own_sem.at[1 + way]))

    for copy in both:
        copy.start()

    @pl.when(late)
    def _():
        for copy in last:
            copy.start()

    @pl.when(jnp.logical_not(late))
    def _():
        for copy in first:
            copy.start()

    for source, target in ((scale_q, out_sq), (scale_k, out_sk), (scale_v, out_sv)):
        target[...] = source[0, :]
    out_norm[...] = norm[...].astype(jnp.bfloat16)
    for copy in both:
        copy.wait()

    @pl.when(late)
    def _():
        for copy in last:
            copy.wait()

    @pl.when(jnp.logical_not(late))
    def _():
        for copy in first:
            copy.wait()


def store(arrays, count):
    cuts = 8
    dma = pltpu.SemaphoreType.DMA
    hbm = pl.BlockSpec(memory_space=pltpu.HBM)
    vmem = pl.BlockSpec(memory_space=pltpu.VMEM)
    return pl.pallas_call(
        functools.partial(store_kernel, count, cuts),
        in_specs=[vmem] * (len(arrays) - 1) + [hbm],
        out_specs=[hbm] * 5 + [vmem] * 4,
        out_shape=[jax.ShapeDtypeStruct(a.shape, a.dtype) for a in arrays[:5]]
        + [jax.ShapeDtypeStruct((a.shape[1],), a.dtype) for a in arrays[5:8]]
        + [jax.ShapeDtypeStruct(arrays[8].shape, jnp.bfloat16)],
        scratch_shapes=[dma((5, cuts)), dma((2 * count,)), dma((3,))],
        compiler_params=pltpu.CompilerParams(vmem_limit_bytes=2 * arrays[-1].size + 2**20),
    )(*arrays)


def store_one_kernel(cuts, source, target, sem):
    copies = pieces_of(source, target, sem, cuts)
    for copy in copies:
        copy.start()
    for copy in copies:
        copy.wait()


def store_one(array):
    cuts = 8
    return pl.pallas_call(
        functools.partial(store_one_kernel, cuts),
        in_specs=[pl.BlockSpec(memory_space=pltpu.VMEM)],
        out_specs=pl.BlockSpec(memory_space=pltpu.HBM),
        out_shape=jax.ShapeDtypeStruct(array.shape, array.dtype),
        scratch_shapes=[pltpu.SemaphoreType.DMA((cuts,))],
        compiler_params=pltpu.CompilerParams(vmem_limit_bytes=2**20),
    )(array)


def late_kernel(count, half, tile, own_k, own_v, after, rk, rv, load_sem, send_sem, recv_sem):
    me, node = ring_of(count)
    side = lax.axis_index("width")
    ahead, behind = node(1), node(-1)
    cut = cut_of(half)
    rest = half - cut
    pieces = [(rk, rest, t * tile) for t in range(rest // tile)]
    pieces += [(rv, half, t * tile) for t in range(half // tile)]

    def ring_copy(owner, step, p, way):
        ref, size, first = pieces[p]
        piece = ref.at[pl.ds(pl.multiple_of((owner * 2 + way) * size + first, 16), tile)]
        return pltpu.make_async_remote_copy(
            src_ref=piece, dst_ref=piece,
            send_sem=send_sem.at[way, lax.rem(step, 2)], recv_sem=recv_sem.at[way, lax.rem(step, 3), p],
            device_id=(behind if way else ahead, side), device_id_type=MESH,
        )

    def owner_of(step, way):
        return node(step if way else -step)

    def leave(step):
        whole = rv.at[pl.ds(0, rest + half)]
        for way in range(2):
            pltpu.make_async_remote_copy(
                src_ref=whole, dst_ref=whole, send_sem=send_sem.at[way, lax.rem(step, 2)],
                recv_sem=recv_sem.at[way, 0, 0], device_id=(ahead, side), device_id_type=MESH,
            ).wait_send()

    @pl.when(lax.rem(side, 2) == 1)
    def _():
        barrier = pltpu.get_barrier_semaphore()
        for other in (ahead, behind):
            pl.semaphore_signal(barrier, inc=1, device_id=(other, side), device_id_type=MESH)
        loads = []
        for way in range(2):
            there = pl.ds(pl.multiple_of((me * 2 + way) * half + cut, 16), rest)
            here = pl.ds(pl.multiple_of((me * 2 + way) * rest, 16), rest)
            loads.append(pltpu.make_async_copy(own_k.at[there], rk.at[here], load_sem.at[0, way]))
            at = pl.ds(pl.multiple_of((me * 2 + way) * half, 16), half)
            loads.append(pltpu.make_async_copy(own_v.at[at], rv.at[at], load_sem.at[1, way]))
        for load in loads:
            load.start()
        for load in loads:
            load.wait()
        pl.semaphore_wait(barrier, 2)
        for p in range(len(pieces)):
            for way in range(2):
                ring_copy(me, 0, p, way).start()

        def forward(step, carry):
            for p in range(len(pieces)):
                for way in range(2):
                    ring_copy(owner_of(step, way), step - 1, p, way).wait_recv()
                    ring_copy(owner_of(step, way), step, p, way).start()
            leave(step - 1)
            return carry

        lax.fori_loop(1, count - 1, forward, 0)
        for p in range(len(pieces)):
            for way in range(2):
                ring_copy(owner_of(count - 1, way), count - 2, p, way).wait_recv()
        leave(count - 2)


def gather_late(own_k, own_v, after, count):
    half = own_k.shape[0] // count // 2
    rest = half - cut_of(half)
    tile = rest if half % 112 == 0 else 16
    n = (rest + half) // tile
    hbm = pl.BlockSpec(memory_space=pltpu.HBM)
    vmem = pl.BlockSpec(memory_space=pltpu.VMEM)
    dma = pltpu.SemaphoreType.DMA
    return pl.pallas_call(
        functools.partial(late_kernel, count, half, tile),
        in_specs=[hbm] * 3,
        out_specs=[vmem] * 2,
        out_shape=[
            pltpu.VMEM((2 * count * rest, own_k.shape[1]), own_k.dtype),
            pltpu.VMEM(own_v.shape, own_v.dtype),
        ],
        scratch_shapes=[dma((2, 2)), dma((2, 2)), dma((2, 3, n))],
        compiler_params=pltpu.CompilerParams(
            collective_id=1, has_side_effects=True, vmem_limit_bytes=56 * 2**20
        ),
    )(own_k, own_v, after)


def store_late_kernel(count, rk, rv, start_k, start_v, out_k, out_v, sem):
    me, side = lax.axis_index("zero"), lax.axis_index("width")
    rows, rest = rv.shape[0] // count, rk.shape[0] // count // 2
    half = rows // 2

    @pl.when(lax.rem(side, 2) == 1)
    def _():
        for k in range(1, count):
            owner = lax.rem(me + k, count)
            at = pl.ds(pl.multiple_of(owner * rows, 16), rows)
            pltpu.make_async_copy(rv.at[at], out_v.at[at], sem.at[0]).start()
            for way in range(2):
                here = pl.ds(pl.multiple_of((owner * 2 + way) * rest, 16), rest)
                there = pl.ds(pl.multiple_of(owner * rows + way * half + half - rest, 16), rest)
                pltpu.make_async_copy(rk.at[here], out_k.at[there], sem.at[1]).start()
        for i, (near, far) in enumerate(((rv, out_v), (rk, out_k))):
            n = near.shape[0] // count * (count - 1)
            pltpu.make_async_copy(near.at[pl.ds(0, n)], far.at[pl.ds(0, n)], sem.at[i]).wait()


def store_late(rk, rv, start_k, start_v, count):
    hbm = pl.BlockSpec(memory_space=pltpu.HBM)
    vmem = pl.BlockSpec(memory_space=pltpu.VMEM)
    dma = pltpu.SemaphoreType.DMA
    return pl.pallas_call(
        functools.partial(store_late_kernel, count),
        in_specs=[vmem] * 2 + [hbm] * 2,
        out_specs=[hbm] * 2,
        out_shape=[jax.ShapeDtypeStruct(a.shape, a.dtype) for a in (start_k, start_v)],
        scratch_shapes=[dma((2,))],
        input_output_aliases={2: 0, 3: 1},
        compiler_params=pltpu.CompilerParams(vmem_limit_bytes=40 * 2**20),
    )(rk, rv, start_k, start_v)


def solution(mesh):
    count, across = mesh.shape["zero"], mesh.shape["width"]

    def body(
        train_query, slow_query, train_key, slow_key, train_value, slow_value, norm_train, norm_step
    ):
        arrays = gather(
            (train_query, slow_query, train_key, slow_key, train_value, slow_value),
            norm_train, norm_step, count, across,
        )
        rq = store_one(arrays[0])
        rk, rv, lq, lk, lv, *scales, norm = store((*arrays[1:], rq), count)
        serve_norm = norm.reshape(-1)
        rk, rv = store_late(*gather_late(rk, rv, serve_norm, count), rk, rv, count)
        return (rq, rk, rv, *scales, serve_norm, lq, lk, lv)

    in_specs = (P("zero", "width"),) * 6 + (P(("zero", "width")),) * 2
    out_specs = (
        (P(None, "width"),) * 3 + (P("width"),) * 3 + (P(),) + (P("zero", "width"),) * 3
    )
    return jax.shard_map(body, mesh=mesh, in_specs=in_specs, out_specs=out_specs, check_vma=False)
```
